128 devices in a mesh: lat: 16 (over y, z), ch: 8 (over x, core).
Axes of the slice: x: 4, y: 4, z: 4, core: 2. Of those that a mesh axis runs over, the one named last changes fastest.
Arguments:
- field_in: bfloat16 [768, 384, 768], P('ch', 'lat'), may hold values from -80 to 80
- ln_gain: float32 [2, 768], P(None, 'ch'), may hold values from 0.5 to 1.5
- ln_shift: float32 [2, 768], P(None, 'ch'), may hold values from -1.5 to 1.5
- mix_first: bfloat16 [2, 2, 8, 96, 96], P(None, None, 'ch'), may hold values from -0.4375 to 0.4375
- mix_bias: bfloat16 [2, 2, 8, 96], P(None, None, 'ch'), may hold values from -3 to 3
- mix_second: bfloat16 [2, 2, 8, 96, 96], P(None, None, 'ch'), may hold values from -0.4375 to 0.4375
Outputs:
- field_out: bfloat16 [768, 384, 768], P('ch', 'lat')
The draws below stay inside these ranges and needn't reach their ends.
All inputs are finite; a program needn't handle non-finite values.
Results may differ from the reference program's by a relative error of at most 0.014.
Values may be sent and summed in bfloat16 or wider, within the bound.
No kernel may reach another device: no remote copies, remote signals or barrier semaphores. Data moves between devices by JAX's collectives and lax.ppermute only.
A program may use at most 128 MiB of HBM per device.

```python
import math
import jax
import jax.numpy as jnp
from jax import lax

BLOCKS = 8
BLOCK = 96
CH = 768
LAT = 384
LON = 768
MODES = 384
LAYERS = 2


def draw_field_in(key, part):
    subkeys = jax.random.split(key, 4)
    base_draw = jnp.clip(jax.random.normal(subkeys[0], (CH, LAT, LON), jnp.float32), -5.0, 5.0)
    trend_rate = math.log(3.0)
    row_pos = jnp.arange(LAT, dtype=jnp.float32) / (LAT - 1)
    chan_pos = jnp.arange(CH, dtype=jnp.float32) / (CH - 1)
    row_scale = jnp.exp(trend_rate * (row_pos - 0.5) + jax.random.uniform(subkeys[1], (LAT,), jnp.float32, -0.6, 0.6))
    chan_scale = jnp.exp(trend_rate * (chan_pos - 0.5) + jax.random.uniform(subkeys[2], (CH,), jnp.float32, -0.6, 0.6))
    col_scale = jnp.exp(jax.random.uniform(subkeys[3], (LON,), jnp.float32, -0.4, 0.4))
    scaled = base_draw * chan_scale[:, None, None] * row_scale[None, :, None] * col_scale[None, None, :]
    return scaled.astype(jnp.bfloat16)


def level_of(key, shape, shards, least, top_value):
    level = 1.0
    for dim, blocks in shards:
        steps = jax.random.uniform(jax.random.fold_in(jax.random.fold_in(key, 6), dim), (blocks,), jnp.float32, least / len(shards), top_value / len(shards))
        level = level * jnp.repeat(jnp.exp(steps), shape[dim] // blocks).reshape((-1,) + (1,) * (len(shape) - 1 - dim))
    return level


def noise(stream_key, dims, scale, most, shards=(), held_as=jnp.bfloat16):
    entries = scale * jax.random.normal(stream_key, dims, jnp.float32)
    if shards:
        entries = entries * level_of(stream_key, dims, shards, -0.22, 0.18)
    return jnp.clip(entries, -most, most).astype(held_as)


def setup_inputs(seed: int = 0) -> dict:
    arg_keys = jax.random.split(jax.random.key(seed), 7)
    field_in = draw_field_in(jax.random.fold_in(arg_keys[6], 71), 0)
    ln_gain = jnp.clip(1.0 + 0.1 * jax.random.normal(arg_keys[1], (LAYERS, CH), jnp.float32), 0.5, 1.5)
    ln_shift = noise(arg_keys[2], (LAYERS, CH), 0.3, 1.5, ((1, 8),), jnp.float32)
    mix_first = noise(arg_keys[3], (LAYERS, 2, BLOCKS, BLOCK, BLOCK), (2 * BLOCK) ** -0.5, 0.4375, ((2, 8),))
    mix_bias = noise(arg_keys[4], (LAYERS, 2, BLOCKS, BLOCK), 0.5, 3.0, ((2, 8),))
    mix_second = noise(arg_keys[5], (LAYERS, 2, BLOCKS, BLOCK, BLOCK), (2 * BLOCK) ** -0.5, 0.4375, ((2, 8),))
    return {"field_in": field_in, "ln_gain": ln_gain, "ln_shift": ln_shift, "mix_first": mix_first, "mix_bias": mix_bias, "mix_second": mix_second}


norm_eps = 1e-05
shrink_level = 0.01

def trig_pair(length, freq_count):
    positions = jnp.arange(length, dtype=jnp.int32)
    freq_ids = jnp.arange(freq_count, dtype=jnp.int32)
    phase_ids = positions[:, None] * freq_ids[None, :] % length
    angles = phase_ids.astype(jnp.float32) * (2.0 * math.pi / length)
    norm_scale = 1.0 / math.sqrt(length)
    return ((jnp.cos(angles) * norm_scale).astype(jnp.bfloat16), (jnp.sin(angles) * norm_scale).astype(jnp.bfloat16))

def soft_shrink(values):
    return jnp.sign(values) * jnp.maximum(jnp.abs(values) - shrink_level, 0.0)

def reference(field_in, ln_gain, ln_shift, mix_first, mix_bias, mix_second):
    lon_cos, lon_sin = trig_pair(LON, MODES)
    lat_cos, lat_sin = trig_pair(LAT, LAT)
    cos_rows = lat_cos.astype(jnp.float32)
    sin_rows = lat_sin.astype(jnp.float32)
    mode_weight = jnp.where(jnp.arange(MODES) == 0, 1.0, 2.0).astype(jnp.float32)
    inv_cos = lon_cos.astype(jnp.float32) * mode_weight[None, :]
    inv_sin = lon_sin.astype(jnp.float32) * mode_weight[None, :]
    fwd_cos = lon_cos.astype(jnp.float32)
    fwd_sin = lon_sin.astype(jnp.float32)

    def block_filter(inputs):
        normed_block, first_w, first_b, second_w = inputs
        source = normed_block.astype(jnp.float32)
        lon_re = jnp.einsum('chw,wk->chk', source, fwd_cos).astype(jnp.bfloat16).astype(jnp.float32)
        lon_im = (-jnp.einsum('chw,wk->chk', source, fwd_sin)).astype(jnp.bfloat16).astype(jnp.float32)
        spec_re = (jnp.einsum('hj,chk->cjk', cos_rows, lon_re) + jnp.einsum('hj,chk->cjk', sin_rows, lon_im)).astype(jnp.bfloat16).astype(jnp.float32)
        spec_im = (jnp.einsum('hj,chk->cjk', cos_rows, lon_im) - jnp.einsum('hj,chk->cjk', sin_rows, lon_re)).astype(jnp.bfloat16).astype(jnp.float32)
        first_re = first_w[0].astype(jnp.float32)
        first_im = first_w[1].astype(jnp.float32)
        bias_f = first_b.astype(jnp.float32)
        hid_re = jax.nn.relu(jnp.einsum('cjk,cd->djk', spec_re, first_re) - jnp.einsum('cjk,cd->djk', spec_im, first_im) + bias_f[0][:, None, None])
        hid_im = jax.nn.relu(jnp.einsum('cjk,cd->djk', spec_im, first_re) + jnp.einsum('cjk,cd->djk', spec_re, first_im) + bias_f[1][:, None, None])
        hid_re = hid_re.astype(jnp.bfloat16).astype(jnp.float32)
        hid_im = hid_im.astype(jnp.bfloat16).astype(jnp.float32)
        second_re = second_w[0].astype(jnp.float32)
        second_im = second_w[1].astype(jnp.float32)
        mix_re = soft_shrink(jnp.einsum('cjk,cd->djk', hid_re, second_re) - jnp.einsum('cjk,cd->djk', hid_im, second_im))
        mix_im = soft_shrink(jnp.einsum('cjk,cd->djk', hid_im, second_re) + jnp.einsum('cjk,cd->djk', hid_re, second_im))
        mix_re = mix_re.astype(jnp.bfloat16).astype(jnp.float32)
        mix_im = mix_im.astype(jnp.bfloat16).astype(jnp.float32)
        back_re = (jnp.einsum('jh,cjk->chk', cos_rows, mix_re) - jnp.einsum('jh,cjk->chk', sin_rows, mix_im)).astype(jnp.bfloat16).astype(jnp.float32)
        back_im = (jnp.einsum('jh,cjk->chk', cos_rows, mix_im) + jnp.einsum('jh,cjk->chk', sin_rows, mix_re)).astype(jnp.bfloat16).astype(jnp.float32)
        return jnp.einsum('chk,wk->chw', back_re, inv_cos) - jnp.einsum('chk,wk->chw', back_im, inv_sin)
    row_pos = jnp.arange(LAT, dtype=jnp.float32)
    area_weights = jnp.cos((row_pos + 0.5) * (math.pi / LAT) - 0.5 * math.pi)[None, :, None]
    current = field_in
    source = field_in.astype(jnp.float32)
    target = jnp.sum(area_weights * source * source)
    for layer_idx in range(LAYERS):
        total_sum = lax.optimization_barrier(jnp.sum(source, axis=0))
        squares = lax.optimization_barrier(jnp.sum(source * source, axis=0))
        mean_val = total_sum / CH
        spread = squares / CH - mean_val * mean_val
        inv_std = lax.rsqrt(spread + norm_eps)
        gain_col = ln_gain[layer_idx].astype(jnp.float32)[:, None, None]
        shift_col = ln_shift[layer_idx].astype(jnp.float32)[:, None, None]
        normed = ((source - mean_val) * inv_std * gain_col + shift_col).astype(jnp.bfloat16)
        blocks_in = normed.reshape(BLOCKS, BLOCK, LAT, LON)
        first_w = jnp.moveaxis(mix_first[layer_idx], 1, 0)
        first_b = jnp.moveaxis(mix_bias[layer_idx], 1, 0)
        second_w = jnp.moveaxis(mix_second[layer_idx], 1, 0)
        spatial = lax.map(block_filter, (blocks_in, first_w, first_b, second_w)).reshape(CH, LAT, LON)
        summed = spatial + normed.astype(jnp.float32) + current.astype(jnp.float32)
        energy = jnp.sum(area_weights * summed * summed)
        current = (summed * jnp.sqrt(target / energy)).astype(jnp.bfloat16)
        source = current.astype(jnp.float32)
    return current
```

```python
import functools
import math

import jax
import jax.numpy as jnp
import numpy as np
from jax import lax
from jax.experimental import pallas as pl
from jax.experimental.pallas import tpu as pltpu
from jax.sharding import Mesh
from jax.sharding import PartitionSpec as P

CH = ("ch_0", "ch_1")
LAT = ("lat_0", "lat_1")
LAT_CH = LAT + CH
NORM_EPS = 1e-05


def host_tables():
    def trig(length, freqs):
        n = np.arange(length)
        a = (n[:, None] * freqs[None, :] % length) * (2.0*math.pi/length)
        s = 1.0/math.sqrt(length)
        bf = jnp.bfloat16
        return (np.cos(a)*s).astype(bf), (np.sin(a)*s).astype(bf)
    c, s = trig(384, np.arange(384))
    tf = np.concatenate([c, s], 1)
    re = np.concatenate([c.T, -s.T], 1).reshape(16, 24, 768)
    im = np.concatenate([s.T, c.T], 1).reshape(16, 24, 768)
    ti = np.stack([re, im], 1).reshape(768, 768)
    lc, ls = trig(768, np.arange(384))
    t = np.concatenate([lc.T, -ls.T], 0)
    return tf, ti, t


def exchange_into(xs, unit, put):
    for c in range(len(xs)):
        put(c, jnp.concatenate([x[:, unit*c:unit*(c+1)] for x in xs], axis=1))

def dot(a, b, dims=((1,),(0,))):
    return lax.dot_general(a, b, (dims, ((),())), preferred_element_type=jnp.float32)

def spectral_kernel(r_ref, w1_ref, b1_ref, w2_ref, tf_ref, ti_ref, o_ref, g_ref, f_ref, h_ref):
    n_band, rows, lanes = r_ref.shape
    groups = lanes // 384
    def forward(g, _):
        l = pl.ds(pl.multiple_of(g*384, 384), 384)
        for t in range(rows//16):
            xs = [r_ref[p, 16*t:16*t+16, l] for p in range(16)]
            def put(c, v, t=t):
                g_ref[48*c+16*t:48*c+16*t+16, :] = v
            exchange_into(xs, 24, put)
        prod = dot(g_ref[...], tf_ref[...]).reshape(16, 48, 768)
        re, im = prod[:, :24], prod[:, 24:]
        row = pl.ds(pl.multiple_of(g*384, 384), 384)
        for k in range(3):
            a, b = slice(128*k, 128*k+128), slice(384+128*k, 512+128*k)
            f_ref[k, row, :] = (re[:, :, a] + im[:, :, b]).reshape(384, 128)
            f_ref[3+k, row, :] = (im[:, :, a] - re[:, :, b]).reshape(384, 128)
        return 0
    lax.fori_loop(0, groups, forward, 0)
    def mix(q, _):
        row = pl.ds(q, 96, stride=24)
        s = jnp.concatenate([jnp.concatenate([f_ref[3*part+k, row, :].astype(jnp.bfloat16) for k in range(3)], axis=1) for part in range(2)], axis=0)
        hid = jnp.maximum(dot(w1_ref[...], s) + b1_ref[...], 0.0).astype(jnp.bfloat16)
        out = dot(w2_ref[...], hid)
        out = jnp.where(out > 0.01, out - 0.01, jnp.where(out < -0.01, out + 0.01, 0.0))
        for part in range(2):
            for k in range(3):
                h_ref[3*part+k, row, :] = out[96*part:96*part+96, 128*k:128*k+128]
        return 0
    lax.fori_loop(0, 24, mix, 0)
    def inverse(g, _):
        row = pl.ds(pl.multiple_of(g*384, 384), 384)
        hb = jnp.concatenate([h_ref[k, row, :].astype(jnp.bfloat16) for k in range(6)], axis=1)
        out = dot(ti_ref[...], hb, ((1,),(1,)))
        o_ref[:, :, row] = out.astype(jnp.bfloat16).reshape(16, 48, 384)
        return 0
    lax.fori_loop(0, groups, inverse, 0)

def spectral(r, w1, b1, w2, tf, ti):
    vm = pl.BlockSpec(memory_space=pltpu.VMEM)
    return pl.pallas_call(spectral_kernel, out_shape=jax.ShapeDtypeStruct((16,48,2304), jnp.bfloat16),
        in_specs=[vm]*6, out_specs=vm,
        scratch_shapes=[pltpu.VMEM((768,384), jnp.bfloat16), pltpu.VMEM((6,2304,128), jnp.float32), pltpu.VMEM((6,2304,128), jnp.float32)],
        compiler_params=pltpu.CompilerParams(vmem_limit_bytes=60<<20),
        cost_estimate=pl.CostEstimate(flops=12*10**9, bytes_accessed=10**7, transcendentals=0), name="spectral")(r, w1, b1, w2, tf, ti)

def spatial_kernel(scale_ref, y_ref, v_ref, n_ref, area_ref, tl_ref, u_ref, sum_ref, sq_ref, z_ref):
    g = pl.program_id(0)
    mask = jnp.where(lax.broadcasted_iota(jnp.int32, (1, 384), 1) == 0, 1.0, 2.0)
    for t in range(3):
        xs = [y_ref[p, 16*t:16*t+16, :] for p in range(16)]
        def put(c, v, t=t):
            z_ref[48*c+16*t:48*c+16*t+16, :] = v.astype(jnp.float32) * mask
        exchange_into(xs, 24, put)
    z = z_ref[...].reshape(16, 48, 384)
    lhs = jnp.concatenate([z[:, :24], z[:, 24:]], axis=2).reshape(384, 768).astype(jnp.bfloat16)
    sp = dot(lhs, tl_ref[...]).reshape(16, 24, 768)
    u = sp + n_ref[...].astype(jnp.float32) + v_ref[...].astype(jnp.float32) * scale_ref[0]
    u_ref[...] = u.astype(jnp.bfloat16)
    @pl.when(g == 0)
    def _():
        sum_ref[...] = jnp.zeros_like(sum_ref)
        sq_ref[...] = jnp.zeros_like(sq_ref)
    sum_ref[...] += jnp.sum(u, axis=0)
    sq_ref[...] += jnp.sum(u * u, axis=0)

def spatial(scale, y, v, n, tl):
    vm = pl.BlockSpec(memory_space=pltpu.VMEM)
    blk = pl.BlockSpec((16,24,768), lambda g: (g,0,0))
    acc = pl.BlockSpec((24,768), lambda g: (0,0))
    return pl.pallas_call(lambda s,y,v,n,t,u,a,b,z: spatial_kernel(s,y,v,n,None,t,u,a,b,z),
        out_shape=(jax.ShapeDtypeStruct((96,24,768), jnp.bfloat16), jax.ShapeDtypeStruct((24,768), jnp.float32), jax.ShapeDtypeStruct((24,768), jnp.float32)),
        grid=(6,),
        in_specs=[pl.BlockSpec(memory_space=pltpu.SMEM), pl.BlockSpec((16,48,384), lambda g: (0,0,g)), blk, blk, pl.BlockSpec((768,768), lambda g: (0,0))],
        out_specs=(blk, acc, acc),
        scratch_shapes=[pltpu.VMEM((768,384), jnp.float32)],
        compiler_params=pltpu.CompilerParams(vmem_limit_bytes=50<<20),
        cost_estimate=pl.CostEstimate(flops=3*10**9, bytes_accessed=15*10**6, transcendentals=0), name="spatial")(scale, y, v, n, tl)


def sum_over(x, axes):
    copies = jnp.broadcast_to(x, (lax.axis_size(axes), *x.shape))
    everything = lax.all_to_all(copies, axes, split_axis=0, concat_axis=0, tiled=True)
    return jnp.sum(everything.astype(jnp.float32), axis=0)


def swap_pieces(x):
    return lax.all_to_all(x, LAT, split_axis=0, concat_axis=0, tiled=True)


def complex_weight(w):
    re, im = w[0].T, w[1].T
    return jnp.concatenate([jnp.concatenate([re, -im], 1), jnp.concatenate([im, re], 1)], 0)


def per_device(field_in, ln_gain, ln_shift, mix_first, mix_bias, mix_second):
    ch_dev, band_rows, lon_cells = field_in.shape
    lat_parts = lax.axis_size(LAT)
    lat_rows = band_rows * lat_parts
    ch_all = ch_dev * lax.axis_size(CH)
    tf, ti, tl = (jnp.asarray(t) for t in host_tables())
    t_forward = tl.reshape(2, lat_parts, 24, lon_cells).transpose(1, 0, 2, 3).reshape(768, lon_cells)
    row_pos = (lax.axis_index(LAT) * band_rows + jnp.arange(band_rows)).astype(jnp.float32)
    area = jnp.cos((row_pos + 0.5) * (math.pi / lat_rows) - 0.5 * math.pi)[:, None]
    source = field_in.astype(jnp.float32)
    sums, squares = jnp.sum(source, axis=0), jnp.sum(source * source, axis=0)
    current, scale = field_in, jnp.float32(1.0)
    target_band = target = None
    for layer in range(mix_first.shape[0]):
        stats = sum_over(jnp.stack([sums, squares]).astype(jnp.bfloat16), CH)
        band = jnp.sum(area * stats[1])
        if layer == 0:
            target_band = band
        else:
            both = jnp.broadcast_to(jnp.stack([target_band, band])[:, None], (2, 128))
            both = sum_over(both, LAT)
            target = both[0, 0]
            scale = jnp.sqrt(target / both[1, 0])
        mean = stats[0] / ch_all
        spread = stats[1] / ch_all - mean * mean
        inv_std = scale * lax.rsqrt(spread * (scale * scale) + NORM_EPS)
        gain, shift = ln_gain[layer][:, None, None], ln_shift[layer][:, None, None]
        normed = ((current.astype(jnp.float32) - mean) * inv_std * gain + shift).astype(jnp.bfloat16)
        lon = dot(t_forward, normed.reshape(ch_dev * band_rows, lon_cells), ((1,), (1,)))
        pieces = swap_pieces(lon.astype(jnp.bfloat16).reshape(lat_parts, 48, ch_dev * band_rows))
        bias = mix_bias[layer, :, 0].astype(jnp.float32).reshape(2 * ch_dev, 1)
        back = spectral(
            pieces,
            complex_weight(mix_first[layer, :, 0]),
            bias,
            complex_weight(mix_second[layer, :, 0]),
            tf,
            ti,
        )
        current, sums, squares = spatial(scale.reshape(1), swap_pieces(back), current, normed, tl)
    energy = sum_over(jnp.broadcast_to(jnp.sum(area * squares), (1, 128)), LAT_CH)[0, 0]
    return (current.astype(jnp.float32) * jnp.sqrt(target / energy)).astype(jnp.bfloat16)


def solution(mesh):
    finer = Mesh(mesh.devices.reshape(4, 4, 4, 2), LAT_CH)
    in_specs = (
        P(CH, LAT, None),
        P(None, CH),
        P(None, CH),
        P(None, None, CH, None, None),
        P(None, None, CH, None),
        P(None, None, CH, None, None),
    )
    return jax.shard_map(
        per_device, mesh=finer, in_specs=in_specs, out_specs=P(CH, LAT, None), check_vma=False
    )
```

```python
import functools
import math

import jax
import jax.numpy as jnp
import numpy as np
from jax import lax
from jax.experimental import pallas as pl
from jax.experimental.pallas import tpu as pltpu
from jax.sharding import Mesh
from jax.sharding import PartitionSpec as P

CH = ("ch_0", "ch_1")
LAT = ("lat_0", "lat_1")
LAT_CH = LAT + CH
NORM_EPS = 1e-05


def host_tables():
    def trig(length, freqs):
        n = np.arange(length)
        a = (n[:, None] * freqs[None, :] % length) * (2.0*math.pi/length)
        s = 1.0/math.sqrt(length)
        bf = jnp.bfloat16
        return (np.cos(a)*s).astype(bf), (np.sin(a)*s).astype(bf)
    c, s = trig(384, np.arange(384))
    tf = np.concatenate([c, s], 1)
    re = np.concatenate([c.T, -s.T], 1).reshape(16, 24, 768)
    im = np.concatenate([s.T, c.T], 1).reshape(16, 24, 768)
    ti = np.stack([re, im], 1).reshape(768, 768)
    lc, ls = trig(768, np.arange(384))
    t = np.concatenate([lc.T, -ls.T], 0)
    return tf, ti, t


MIX_STEP = 8
SPECTRAL_VMEM = 36 << 20
SPATIAL_VMEM = 28 << 20
NORM_VMEM = 24 << 20


def exchange_into(xs, unit, put):
    for c in range(len(xs)):
        put(c, jnp.concatenate([x[:, unit*c:unit*(c+1)] for x in xs], axis=1))

def dot(a, b, dims=((1,),(0,))):
    return lax.dot_general(a, b, (dims, ((),())), preferred_element_type=jnp.float32)

def complex_weight(w_ref):
    re, im = (w_ref[part, 0].astype(jnp.float32).T for part in range(2))
    rows = [jnp.concatenate([re, -im], axis=1), jnp.concatenate([im, re], axis=1)]
    return jnp.concatenate(rows, axis=0).astype(jnp.bfloat16)


def spectral_kernel(r_ref, wa_ref, ba_ref, wb_ref, tf_hbm, ti_hbm, o_ref, g_ref, f_ref, h_ref, tf_ref, ti_ref, sems):
    load_tf = pltpu.make_async_copy(tf_hbm, tf_ref, sems.at[0])
    load_ti = pltpu.make_async_copy(ti_hbm, ti_ref, sems.at[1])
    load_tf.start()
    load_ti.start()
    w1, w2 = complex_weight(wa_ref), complex_weight(wb_ref)
    b1 = jnp.concatenate([ba_ref[part].astype(jnp.float32).reshape(1, -1).T for part in range(2)], axis=0)
    load_tf.wait()
    groups = r_ref.shape[2] // 384

    def forward(g, _):
        l = pl.ds(pl.multiple_of(g * 384, 384), 384)
        for t in range(3):
            def put(c, v, t=t):
                g_ref[48 * c + 16 * t : 48 * c + 16 * t + 16, :] = v

            exchange_into([r_ref[p, 16 * t : 16 * t + 16, l] for p in range(16)], 24, put)
        prod = dot(g_ref[...], tf_ref[...]).reshape(16, 48, 768)
        re, im = prod[:, :24], prod[:, 24:]
        for k in range(3):
            a, b = slice(128 * k, 128 * k + 128), slice(384 + 128 * k, 512 + 128 * k)
            f_ref[k, l, :] = (re[:, :, a] + im[:, :, b]).reshape(384, 128)
            f_ref[3 + k, l, :] = (im[:, :, a] - re[:, :, b]).reshape(384, 128)
        return 0

    def mix(i, _):
        rows = [pl.ds(i * MIX_STEP + k, 96, stride=24) for k in range(MIX_STEP)]
        s = jnp.concatenate(
            [
                jnp.concatenate(
                    [f_ref[3 * part + k, row, :].astype(jnp.bfloat16) for row in rows for k in range(3)], axis=1
                )
                for part in range(2)
            ],
            axis=0,
        )
        hid = jnp.maximum(dot(w1, s) + b1, 0.0).astype(jnp.bfloat16)
        out = dot(w2, hid)
        out = jnp.where(out > 0.01, out - 0.01, jnp.where(out < -0.01, out + 0.01, 0.0))
        for n, row in enumerate(rows):
            for part in range(2):
                for k in range(3):
                    lane = 384 * n + 128 * k
                    h_ref[3 * part + k, row, :] = out[96 * part : 96 * part + 96, lane : lane + 128]
        return 0

    def inverse(g, _):
        row = pl.ds(pl.multiple_of(g * 384, 384), 384)
        hb = jnp.concatenate([h_ref[k, row, :].astype(jnp.bfloat16) for k in range(6)], axis=1)
        out = dot(ti_ref[...], hb, ((1,), (1,)))
        o_ref[:, :, row] = out.astype(jnp.bfloat16).reshape(16, 48, 384)
        return 0

    lax.fori_loop(0, groups, forward, 0, unroll=3)
    lax.fori_loop(0, 24 // MIX_STEP, mix, 0)
    load_ti.wait()
    lax.fori_loop(0, groups, inverse, 0, unroll=2)


def spectral(r, wa, ba, wb, tf, ti):
    vm, hbm = pl.BlockSpec(memory_space=pltpu.VMEM), pl.BlockSpec(memory_space=pltpu.HBM)
    return pl.pallas_call(
        spectral_kernel,
        out_shape=jax.ShapeDtypeStruct(r.shape, jnp.bfloat16),
        in_specs=[vm] * 4 + [hbm] * 2,
        out_specs=vm,
        scratch_shapes=[
            pltpu.VMEM((768, 384), jnp.bfloat16),
            pltpu.VMEM((6, 2304, 128), jnp.float32),
            pltpu.VMEM((6, 2304, 128), jnp.float32),
            pltpu.VMEM(tf.shape, tf.dtype),
            pltpu.VMEM(ti.shape, ti.dtype),
            pltpu.SemaphoreType.DMA((2,)),
        ],
        compiler_params=pltpu.CompilerParams(vmem_limit_bytes=SPECTRAL_VMEM),
        cost_estimate=pl.CostEstimate(flops=12 * 10**9, bytes_accessed=10**7, transcendentals=0),
        name="spectral",
    )(r, wa, ba, wb, tf, ti)


def spatial_kernel(last, scale_ref, y_ref, v_ref, n_ref, tl_ref, u_ref, st_ref, z_ref, sum_ref, sq_ref):
    mask = jnp.where(lax.broadcasted_iota(jnp.int32, (1, 384), 1) == 0, 1.0, 2.0)
    sum_ref[...] = jnp.zeros_like(sum_ref)
    sq_ref[...] = jnp.zeros_like(sq_ref)

    def inverse(g, _):
        l = pl.ds(pl.multiple_of(g * 384, 384), 384)
        for t in range(3):
            def put(c, v, t=t):
                z_ref[48 * c + 16 * t : 48 * c + 16 * t + 16, :] = v.astype(jnp.float32) * mask

            exchange_into([y_ref[p, 16 * t : 16 * t + 16, l] for p in range(16)], 24, put)
        z = z_ref[...].reshape(16, 48, 384)
        lhs = jnp.concatenate([z[:, :24], z[:, 24:]], axis=2).reshape(384, 768).astype(jnp.bfloat16)
        sp = dot(lhs, tl_ref[...]).reshape(16, 24, 768)
        d = pl.ds(pl.multiple_of(g * 16, 16), 16)
        u = sp + n_ref[d].astype(jnp.float32) + v_ref[d].astype(jnp.float32) * scale_ref[0]
        u_ref[d] = u.astype(jnp.bfloat16)
        sum_ref[...] += jnp.sum(u, axis=0)
        sq_ref[...] += jnp.sum(u * u, axis=0)
        return 0

    lax.fori_loop(0, 6, inverse, 0, unroll=2)
    if last:
        st_ref[...] = sq_ref[...]
    else:
        put_stats(st_ref, sum_ref[...], sq_ref[...])


def put_stats(st_ref, sums, squares):
    for dest in range(st_ref.shape[0]):
        st_ref[dest, 0] = sums.astype(jnp.bfloat16)
        st_ref[dest, 1] = squares.astype(jnp.bfloat16)


def spatial(scale, y, v, n, tl, last):
    vm = pl.BlockSpec(memory_space=pltpu.VMEM)
    plane = v.shape[1:]
    stats = jax.ShapeDtypeStruct(plane, jnp.float32) if last else jax.ShapeDtypeStruct((8, 2, *plane), jnp.bfloat16)

    def body(*refs):
        spatial_kernel(last, *refs)

    return pl.pallas_call(
        body,
        out_shape=(jax.ShapeDtypeStruct(v.shape, jnp.bfloat16), stats),
        in_specs=[pl.BlockSpec(memory_space=pltpu.SMEM)] + [vm] * 4,
        out_specs=(vm, vm),
        scratch_shapes=[pltpu.VMEM((768, 384), jnp.float32), pltpu.VMEM(plane, jnp.float32), pltpu.VMEM(plane, jnp.float32)],
        compiler_params=pltpu.CompilerParams(vmem_limit_bytes=SPATIAL_VMEM),
        cost_estimate=pl.CostEstimate(flops=3 * 10**9, bytes_accessed=15 * 10**6, transcendentals=0),
        name="spatial",
    )(scale, y, v, n, tl)


def stats_kernel(v_ref, st_ref, sum_ref, sq_ref):
    g = pl.program_id(0)

    @pl.when(g == 0)
    def _():
        sum_ref[...] = jnp.zeros_like(sum_ref)
        sq_ref[...] = jnp.zeros_like(sq_ref)

    v = v_ref[...].astype(jnp.float32)
    sum_ref[...] += jnp.sum(v, axis=0)
    sq_ref[...] += jnp.sum(v * v, axis=0)

    @pl.when(g == pl.num_programs(0) - 1)
    def _():
        put_stats(st_ref, sum_ref[...], sq_ref[...])


def first_stats(v):
    plane = v.shape[1:]
    return pl.pallas_call(
        stats_kernel,
        out_shape=jax.ShapeDtypeStruct((8, 2, *plane), jnp.bfloat16),
        grid=(4,),
        in_specs=[pl.BlockSpec((24, *plane), lambda g: (g, 0, 0))],
        out_specs=pl.BlockSpec((8, 2, *plane), lambda g: (0, 0, 0, 0)),
        scratch_shapes=[pltpu.VMEM(plane, jnp.float32), pltpu.VMEM(plane, jnp.float32)],
        compiler_params=pltpu.CompilerParams(vmem_limit_bytes=16 << 20),
        cost_estimate=pl.CostEstimate(flops=6 * 10**6, bytes_accessed=4 * 10**6, transcendentals=0),
        name="first_stats",
    )(v)


def norm_kernel(scale_ref, gain_ref, shift_ref, v_ref, st_ref, tw_ref, n_ref, o_ref, mean_ref, inv_ref):
    ch_all = 768
    scale = scale_ref[0]
    total, squares = st_ref[0].astype(jnp.float32), st_ref[1].astype(jnp.float32)
    mean = total / ch_all
    spread = squares / ch_all - mean * mean
    mean_ref[...] = mean
    inv_ref[...] = scale * lax.rsqrt(spread * (scale * scale) + NORM_EPS)

    def group(g, _):
        mean, inv = mean_ref[...], inv_ref[...]
        rows = []
        for i in range(16):
            c = g * 16 + i
            normed = (v_ref[c].astype(jnp.float32) - mean) * inv * gain_ref[c] + shift_ref[c]
            rows.append(normed)
        x = jnp.concatenate(rows, axis=0).astype(jnp.bfloat16)
        n_ref[pl.ds(pl.multiple_of(g * 16, 16), 16)] = x.astype(jnp.float32).reshape(16, 24, 768).astype(jnp.bfloat16)
        out = dot(tw_ref[...], x, ((1,), (1,)))
        o_ref[:, :, pl.ds(pl.multiple_of(g * 384, 384), 384)] = out.astype(jnp.bfloat16).reshape(16, 48, 384)
        return 0

    lax.fori_loop(0, 6, group, 0, unroll=2)


def norm_lon(scale, gain, shift, v, stats, tw):
    vm, sm = pl.BlockSpec(memory_space=pltpu.VMEM), pl.BlockSpec(memory_space=pltpu.SMEM)
    plane = v.shape[1:]
    return pl.pallas_call(
        norm_kernel,
        out_shape=(jax.ShapeDtypeStruct(v.shape, jnp.bfloat16), jax.ShapeDtypeStruct((16, 48, 2304), jnp.bfloat16)),
        in_specs=[sm] * 3 + [vm] * 3,
        out_specs=(vm, vm),
        scratch_shapes=[pltpu.VMEM(plane, jnp.float32), pltpu.VMEM(plane, jnp.float32)],
        compiler_params=pltpu.CompilerParams(vmem_limit_bytes=NORM_VMEM),
        cost_estimate=pl.CostEstimate(flops=3 * 10**9, bytes_accessed=10**7, transcendentals=0),
        name="norm_lon",
    )(scale, gain, shift, v, stats, tw)


def final_kernel(scale_ref, u_ref, o_ref):
    d = pl.ds(pl.multiple_of(pl.program_id(0) * o_ref.shape[0], 8), o_ref.shape[0])
    o_ref[...] = (u_ref[d].astype(jnp.float32) * scale_ref[0]).astype(jnp.bfloat16)


def final_scale(scale, u):
    return pl.pallas_call(
        final_kernel,
        out_shape=jax.ShapeDtypeStruct(u.shape, jnp.bfloat16),
        grid=(6,),
        in_specs=[pl.BlockSpec(memory_space=pltpu.SMEM), pl.BlockSpec(memory_space=pltpu.VMEM)],
        out_specs=pl.BlockSpec((16, *u.shape[1:]), lambda g: (g, 0, 0)),
        compiler_params=pltpu.CompilerParams(vmem_limit_bytes=12 << 20),
        cost_estimate=pl.CostEstimate(flops=10**7, bytes_accessed=7 * 10**6, transcendentals=0),
        name="final_scale",
    )(scale, u)


def sum_over(x, axes):
    copies = jnp.broadcast_to(x, (lax.axis_size(axes), *x.shape))
    everything = lax.all_to_all(copies, axes, split_axis=0, concat_axis=0, tiled=True)
    return jnp.sum(everything.astype(jnp.float32), axis=0)


def swap_pieces(x):
    return lax.all_to_all(x, LAT, split_axis=0, concat_axis=0, tiled=True)


def per_device(field_in, ln_gain, ln_shift, mix_first, mix_bias, mix_second):
    ch_dev, band_rows, lon_cells = field_in.shape
    lat_parts = lax.axis_size(LAT)
    lat_rows = band_rows * lat_parts
    tf, ti, tl = (jnp.asarray(t) for t in host_tables())
    t_forward = tl.reshape(2, lat_parts, 24, lon_cells).transpose(1, 0, 2, 3).reshape(768, lon_cells)
    row_pos = (lax.axis_index(LAT) * band_rows + jnp.arange(band_rows)).astype(jnp.float32)
    area = jnp.cos((row_pos + 0.5) * (math.pi / lat_rows) - 0.5 * math.pi)[:, None]
    current, scale = field_in, jnp.float32(1.0)
    stats = first_stats(field_in)
    target_band = target = None
    layers = mix_first.shape[0]
    for layer in range(layers):
        stats = jnp.sum(lax.all_to_all(stats, CH, split_axis=0, concat_axis=0, tiled=True).astype(jnp.float32), axis=0)
        band = jnp.sum(area * stats[1])
        if layer == 0:
            target_band = band
        else:
            both = jnp.broadcast_to(jnp.stack([target_band, band])[:, None], (2, 128))
            both = sum_over(both, LAT)
            target = both[0, 0]
            scale = jnp.sqrt(target / both[1, 0])
        scale_1 = scale.reshape(1)
        normed, lon = norm_lon(scale_1, ln_gain[layer], ln_shift[layer], current, stats, t_forward)
        back = spectral(swap_pieces(lon), mix_first[layer], mix_bias[layer], mix_second[layer], tf, ti)
        current, stats = spatial(scale_1, swap_pieces(back), current, normed, tl, layer == layers - 1)
    energy = sum_over(jnp.broadcast_to(jnp.sum(area * stats), (1, 128)), LAT_CH)[0, 0]
    return final_scale(jnp.sqrt(target / energy).reshape(1), current)


def solution(mesh):
    finer = Mesh(mesh.devices.reshape(4, 4, 4, 2), LAT_CH)
    in_specs = (
        P(CH, LAT, None),
        P(None, CH),
        P(None, CH),
        P(None, None, CH, None, None),
        P(None, None, CH, None),
        P(None, None, CH, None, None),
    )
    return jax.shard_map(
        per_device, mesh=finer, in_specs=in_specs, out_specs=P(CH, LAT, None), check_vma=False
    )
```

```python
import math

import jax
import jax.numpy as jnp
import numpy as np
from jax import lax
from jax.experimental import pallas as pl
from jax.experimental.pallas import tpu as pltpu
from jax.sharding import Mesh
from jax.sharding import PartitionSpec as P

CH = ("ch_0", "ch_1")
LAT = ("lat_0", "lat_1")
LAT_CH = LAT + CH
NORM_EPS = 1e-05
CH_ALL = 768
GROUPS = 6
MIX_STEP = 8
BIG = 60 << 20
F32, BF16 = jnp.float32, jnp.bfloat16
VM = pl.BlockSpec(memory_space=pltpu.VMEM)
SM = pl.BlockSpec(memory_space=pltpu.SMEM)
HBM = pl.BlockSpec(memory_space=pl.ANY)


def host_tables():
    def trig(length, freqs):
        n = np.arange(length)
        a = (n[:, None] * freqs[None, :] % length) * (2.0*math.pi/length)
        s = 1.0/math.sqrt(length)
        bf = jnp.bfloat16
        return (np.cos(a)*s).astype(bf), (np.sin(a)*s).astype(bf)
    c, s = trig(384, np.arange(384))
    tf = np.concatenate([c, s], 1)
    re = np.concatenate([c.T, -s.T], 1).reshape(16, 24, 768)
    im = np.concatenate([s.T, c.T], 1).reshape(16, 24, 768)
    ti = np.stack([re, im], 1).reshape(768, 768)
    lc, ls = trig(768, np.arange(384))
    t = np.concatenate([lc.T, -ls.T], 0)
    return tf, ti, t


def lanes_of(g):
    return pl.ds(pl.multiple_of(g * 384, 384), 384)


def chans_of(g):
    return pl.ds(pl.multiple_of(g * 16, 16), 16)


def exchange_into(xs, unit, put):
    for c in range(len(xs)):
        put(c, jnp.concatenate([x[:, unit * c : unit * (c + 1)] for x in xs], axis=1))


def dot(a, b, dims=((1,), (0,))):
    return lax.dot_general(a, b, (dims, ((), ())), preferred_element_type=F32)


def params(limit=BIG):
    return pltpu.CompilerParams(vmem_limit_bytes=limit)


def cost(flops, moved):
    return pl.CostEstimate(flops=flops, bytes_accessed=moved, transcendentals=0)


def put_stats(st_ref, sums, squares):
    for dest in range(st_ref.shape[0]):
        st_ref[dest, 0] = sums.astype(BF16)
        st_ref[dest, 1] = squares.astype(BF16)


def first_stats_kernel(v_ref, st_ref, sum_ref, sq_ref):
    g = pl.program_id(0)

    @pl.when(g == 0)
    def _():
        sum_ref[...] = jnp.zeros_like(sum_ref)
        sq_ref[...] = jnp.zeros_like(sq_ref)

    v = v_ref[...].astype(F32)
    sum_ref[...] += jnp.sum(v, axis=0)
    sq_ref[...] += jnp.sum(v * v, axis=0)

    @pl.when(g == pl.num_programs(0) - 1)
    def _():
        put_stats(st_ref, sum_ref[...], sq_ref[...])


def first_stats(v):
    plane = v.shape[1:]
    return pl.pallas_call(
        first_stats_kernel,
        out_shape=jax.ShapeDtypeStruct((8, 2, *plane), BF16),
        grid=(4,),
        in_specs=[pl.BlockSpec((24, *plane), lambda g: (g, 0, 0))],
        out_specs=pl.BlockSpec((8, 2, *plane), lambda g: (0, 0, 0, 0)),
        scratch_shapes=[pltpu.VMEM(plane, F32), pltpu.VMEM(plane, F32)],
        compiler_params=params(),
        cost_estimate=cost(6 * 10**6, 4 * 10**6),
        name="first_stats",
    )(v)


def gather_stats(st_ref):
    return tuple(sum(st_ref[d, i].astype(F32) for d in range(st_ref.shape[0])) for i in range(2))


def band_energy(area, squares):
    return jnp.sum(area * squares, keepdims=True)


def band_kernel(st_ref, area_ref, first_ref, sums_ref, pay_ref):
    total, squares = gather_stats(st_ref)
    sums_ref[0] = total
    sums_ref[1] = squares
    here = jnp.broadcast_to(band_energy(area_ref[...], squares), (1, 128))
    for dest in range(pay_ref.shape[0]):
        pay_ref[dest, 0:1] = first_ref[...]
        pay_ref[dest, 1:2] = here


def band_sums(stats, area, first):
    plane = stats.shape[2:]
    return pl.pallas_call(
        band_kernel,
        out_shape=(jax.ShapeDtypeStruct((2, *plane), F32), jax.ShapeDtypeStruct((16, 2, 128), F32)),
        in_specs=[VM] * 3,
        out_specs=(VM, VM),
        compiler_params=params(8 << 20),
        cost_estimate=cost(10**6, 10**6),
        name="band_sums",
    )(stats, area, first)


def layer_scale(pay_ref):
    both = jnp.sum(pay_ref[...], axis=0)
    return jnp.sqrt(both[0:1] / both[1:2])[0, 0]


def norm_body(layer, scale, total, squares, refs):
    gain_ref, shift_ref, v_hbm, tw_ref, n_hbm, o_hbm, v_ref, n_ref, o_ref, mean_ref, inv_ref, sems = refs
    loads = [pltpu.make_async_copy(v_hbm.at[chans_of(g)], v_ref.at[chans_of(g)], sems.at[g]) for g in range(GROUPS)]
    for load in loads:
        load.start()
    mean = total / CH_ALL
    spread = squares / CH_ALL - mean * mean
    mean_ref[...] = mean
    inv_ref[...] = scale * lax.rsqrt(spread * (scale * scale) + NORM_EPS)
    stores = []
    for g in range(GROUPS):
        loads[g].wait()
        mean, inv = mean_ref[...], inv_ref[...]
        rows = []
        for c in range(16 * g, 16 * g + 16):
            rows.append((v_ref[c].astype(F32) - mean) * inv * gain_ref[layer, c] + shift_ref[layer, c])
        x = jnp.concatenate(rows, axis=0).astype(BF16)
        n_ref[chans_of(g)] = x.astype(F32).reshape(16, 24, 768).astype(BF16)
        out = dot(tw_ref[...], x, ((1,), (1,)))
        o_ref[:, :, lanes_of(g)] = out.astype(BF16).reshape(16, 48, 384)
        for k, (src, dst, at) in enumerate(((n_ref, n_hbm, (chans_of(g),)), (o_ref, o_hbm, (slice(None), slice(None), lanes_of(g))))):
            store = pltpu.make_async_copy(src.at[at], dst.at[at], sems.at[GROUPS * (k + 1) + g])
            store.start()
            stores.append(store)
    for store in stores:
        store.wait()


def norm_first_kernel(gain_ref, shift_ref, v_hbm, tw_ref, st_ref, area_ref, n_hbm, o_hbm, band_ref, *rest):
    total, squares = gather_stats(st_ref)
    band_ref[...] = jnp.broadcast_to(band_energy(area_ref[...], squares), (1, 128))
    norm_body(0, 1.0, total, squares, (gain_ref, shift_ref, v_hbm, tw_ref, n_hbm, o_hbm, *rest))


def norm_later_kernel(layer, gain_ref, shift_ref, v_hbm, tw_ref, sums_ref, pay_ref, n_hbm, o_hbm, *rest):
    scale = layer_scale(pay_ref)
    norm_body(layer, scale, sums_ref[0], sums_ref[1], (gain_ref, shift_ref, v_hbm, tw_ref, n_hbm, o_hbm, *rest))


def norm_lon(layer, gain, shift, v, tw, stats, other):
    plane = v.shape[1:]
    pieces = (16, 48, 2304)
    outs = [jax.ShapeDtypeStruct(v.shape, BF16), jax.ShapeDtypeStruct(pieces, BF16)]
    specs = [HBM, HBM]
    if layer == 0:
        kernel = norm_first_kernel
        outs.append(jax.ShapeDtypeStruct((1, 128), F32))
        specs.append(VM)
    else:

        def kernel(*refs):
            norm_later_kernel(layer, *refs)

    return pl.pallas_call(
        kernel,
        out_shape=tuple(outs),
        in_specs=[SM, SM, HBM, VM, VM, VM],
        out_specs=tuple(specs),
        scratch_shapes=[
            pltpu.VMEM(v.shape, BF16),
            pltpu.VMEM(v.shape, BF16),
            pltpu.VMEM(pieces, BF16),
            pltpu.VMEM(plane, F32),
            pltpu.VMEM(plane, F32),
            pltpu.SemaphoreType.DMA((3 * GROUPS,)),
        ],
        compiler_params=params(),
        cost_estimate=cost(3 * 10**9, 10**7),
        name="norm_lon",
    )(gain, shift, v, tw, stats, other)


def complex_weight(w_ref):
    re, im = (w_ref[part].astype(F32).T for part in range(2))
    rows = [jnp.concatenate([re, -im], axis=1), jnp.concatenate([im, re], axis=1)]
    return jnp.concatenate(rows, axis=0).astype(BF16)


def spectral_kernel(
    layer, r_hbm, wa_hbm, ba_ref, wb_hbm, tf_hbm, ti_hbm, o_hbm,
    r_ref, o_ref, g_ref, f_ref, h_ref, wa_ref, wb_ref, tf_ref, ti_ref, sems, out_sems,
):
    def load(g):
        at = (slice(None), slice(None), lanes_of(g))
        return pltpu.make_async_copy(r_hbm.at[at], r_ref.at[at], sems.at[g])

    def store(g):
        at = (slice(None), slice(None), lanes_of(g))
        return pltpu.make_async_copy(o_ref.at[at], o_hbm.at[at], out_sems.at[g])

    load(0).start()
    tables = [
        pltpu.make_async_copy(src, dst, sems.at[GROUPS + i])
        for i, (src, dst) in enumerate(
            ((tf_hbm, tf_ref), (wa_hbm.at[layer, :, 0], wa_ref), (wb_hbm.at[layer, :, 0], wb_ref), (ti_hbm, ti_ref))
        )
    ]
    tables[0].start()
    for g in range(1, GROUPS):
        load(g).start()
    for table in tables[1:]:
        table.start()
    tables[0].wait()

    def forward(g, _):
        load(g).wait()
        l = lanes_of(g)
        for t in range(3):

            def put(c, v, t=t):
                g_ref[48 * c + 16 * t : 48 * c + 16 * t + 16, :] = v

            exchange_into([r_ref[p, 16 * t : 16 * t + 16, l] for p in range(16)], 24, put)
        prod = dot(g_ref[...], tf_ref[...]).reshape(16, 48, 768)
        re, im = prod[:, :24], prod[:, 24:]
        for k in range(3):
            a, b = slice(128 * k, 128 * k + 128), slice(384 + 128 * k, 512 + 128 * k)
            f_ref[k, l, :] = (re[:, :, a] + im[:, :, b]).reshape(384, 128)
            f_ref[3 + k, l, :] = (im[:, :, a] - re[:, :, b]).reshape(384, 128)
        return 0

    lax.fori_loop(0, GROUPS, forward, 0, unroll=3)
    for table in tables[1:]:
        table.wait()
    w1, w2 = complex_weight(wa_ref), complex_weight(wb_ref)
    b1 = jnp.concatenate([ba_ref[layer, part : part + 1].T for part in range(2)], axis=0)

    def mix(i, _):
        rows = [pl.ds(i * MIX_STEP + k, 96, stride=24) for k in range(MIX_STEP)]
        s = jnp.concatenate(
            [
                jnp.concatenate([f_ref[3 * part + k, row, :].astype(BF16) for row in rows for k in range(3)], axis=1)
                for part in range(2)
            ],
            axis=0,
        )
        hid = jnp.maximum(dot(w1, s) + b1, 0.0).astype(BF16)
        out = dot(w2, hid)
        out = jnp.where(out > 0.01, out - 0.01, jnp.where(out < -0.01, out + 0.01, 0.0))
        for n, row in enumerate(rows):
            for part in range(2):
                for k in range(3):
                    lane = 384 * n + 128 * k
                    h_ref[3 * part + k, row, :] = out[96 * part : 96 * part + 96, lane : lane + 128]
        return 0

    lax.fori_loop(0, 24 // MIX_STEP, mix, 0)

    def inverse(g, _):
        l = lanes_of(g)
        hb = jnp.concatenate([h_ref[k, l, :].astype(BF16) for k in range(6)], axis=1)
        out = dot(ti_ref[...], hb, ((1,), (1,)))
        o_ref[:, :, l] = out.astype(BF16).reshape(16, 48, 384)
        store(g).start()
        return 0

    lax.fori_loop(0, GROUPS, inverse, 0, unroll=2)
    for g in range(GROUPS):
        store(g).wait()


def spectral(layer, r, wa, ba, wb, tf, ti):
    def kernel(*refs):
        spectral_kernel(layer, *refs)

    weight = pltpu.VMEM((2, 96, 96), BF16)
    return pl.pallas_call(
        kernel,
        out_shape=jax.ShapeDtypeStruct(r.shape, BF16),
        in_specs=[HBM, HBM, VM, HBM, HBM, HBM],
        out_specs=HBM,
        scratch_shapes=[
            pltpu.VMEM(r.shape, BF16),
            pltpu.VMEM(r.shape, BF16),
            pltpu.VMEM((768, 384), BF16),
            pltpu.VMEM((6, 2304, 128), F32),
            pltpu.VMEM((6, 2304, 128), F32),
            weight,
            weight,
            pltpu.VMEM(tf.shape, BF16),
            pltpu.VMEM(ti.shape, BF16),
            pltpu.SemaphoreType.DMA((GROUPS + 4,)),
            pltpu.SemaphoreType.DMA((GROUPS,)),
        ],
        compiler_params=params(),
        cost_estimate=cost(12 * 10**9, 10**7),
        name="spectral",
    )(r, wa, ba, wb, tf, ti)


def spatial_kernel(first, last, *refs):
    refs = list(refs)
    pay_ref = None if first else refs.pop(0)
    area_ref = refs.pop(0) if last else None
    y_hbm, v_hbm, n_hbm, tl_hbm, u_hbm, st_ref = refs[:6]
    y_ref, v_ref, n_ref, tl_ref, u_ref, z_ref, sum_ref, sq_ref, sems, out_sems = refs[6:]

    def loads(g):
        at = (slice(None), slice(None), lanes_of(g))
        d = chans_of(g)
        return [
            pltpu.make_async_copy(src, dst, sems.at[k, g])
            for k, (src, dst) in enumerate(
                ((y_hbm.at[at], y_ref.at[at]), (v_hbm.at[d], v_ref.at[d]), (n_hbm.at[d], n_ref.at[d]))
            )
        ]

    def store(g):
        d = chans_of(g)
        return pltpu.make_async_copy(u_ref.at[d], u_hbm.at[d], out_sems.at[g])

    table = pltpu.make_async_copy(tl_hbm, tl_ref, sems.at[3, 0])
    for load in loads(0):
        load.start()
    table.start()
    for g in range(1, GROUPS):
        for load in loads(g):
            load.start()
    scale = 1.0 if first else layer_scale(pay_ref)
    mask = jnp.where(lax.broadcasted_iota(jnp.int32, (1, 384), 1) == 0, 1.0, 2.0)
    sum_ref[...] = jnp.zeros_like(sum_ref)
    sq_ref[...] = jnp.zeros_like(sq_ref)
    table.wait()

    def inverse(g, _):
        for load in loads(g):
            load.wait()
        l = lanes_of(g)
        for t in range(3):

            def put(c, v, t=t):
                z_ref[48 * c + 16 * t : 48 * c + 16 * t + 16, :] = v.astype(F32) * mask

            exchange_into([y_ref[p, 16 * t : 16 * t + 16, l] for p in range(16)], 24, put)
        z = z_ref[...].reshape(16, 48, 384)
        lhs = jnp.concatenate([z[:, :24], z[:, 24:]], axis=2).reshape(384, 768).astype(BF16)
        sp = dot(lhs, tl_ref[...]).reshape(16, 24, 768)
        d = chans_of(g)
        u = sp + n_ref[d].astype(F32) + v_ref[d].astype(F32) * scale
        u_ref[d] = u.astype(BF16)
        sum_ref[...] += jnp.sum(u, axis=0)
        sq_ref[...] += jnp.sum(u * u, axis=0)
        store(g).start()
        return 0

    lax.fori_loop(0, GROUPS, inverse, 0, unroll=2)
    if last:
        st_ref[...] = jnp.broadcast_to(band_energy(area_ref[...], sq_ref[...]).reshape(1, 1, 1), st_ref.shape)
    else:
        put_stats(st_ref, sum_ref[...], sq_ref[...])
    for g in range(GROUPS):
        store(g).wait()


def spatial(first, last, extra, y, v, n, tl):
    plane = v.shape[1:]
    stats = jax.ShapeDtypeStruct((128, 1, 128), F32) if last else jax.ShapeDtypeStruct((8, 2, *plane), BF16)

    def kernel(*refs):
        spatial_kernel(first, last, *refs)

    return pl.pallas_call(
        kernel,
        out_shape=(jax.ShapeDtypeStruct(v.shape, BF16), stats),
        in_specs=[VM] * len(extra) + [HBM] * 4,
        out_specs=(HBM, VM),
        scratch_shapes=[
            pltpu.VMEM(y.shape, BF16),
            pltpu.VMEM(v.shape, BF16),
            pltpu.VMEM(v.shape, BF16),
            pltpu.VMEM(tl.shape, BF16),
            pltpu.VMEM(v.shape, BF16),
            pltpu.VMEM((768, 384), F32),
            pltpu.VMEM(plane, F32),
            pltpu.VMEM(plane, F32),
            pltpu.SemaphoreType.DMA((4, GROUPS)),
            pltpu.SemaphoreType.DMA((GROUPS,)),
        ],
        compiler_params=params(),
        cost_estimate=cost(3 * 10**9, 15 * 10**6),
        name="spatial",
    )(*extra, y, v, n, tl)


def final_kernel(pay_ref, energy_ref, u_ref, o_ref):
    target = jnp.sum(pay_ref[...], axis=0)[0:1]
    energy = jnp.sum(energy_ref[...], axis=0)
    scale = jnp.sqrt(target / energy)[0, 0]
    d = pl.ds(pl.program_id(0) * o_ref.shape[0], o_ref.shape[0])
    o_ref[...] = (u_ref[d].astype(F32) * scale).astype(BF16)


def final_scale(pay, energy, u):
    return pl.pallas_call(
        final_kernel,
        out_shape=jax.ShapeDtypeStruct(u.shape, BF16),
        grid=(6,),
        in_specs=[VM] * 3,
        out_specs=pl.BlockSpec((16, *u.shape[1:]), lambda g: (g, 0, 0)),
        compiler_params=params(12 << 20),
        cost_estimate=cost(10**7, 7 * 10**6),
        name="final_scale",
    )(pay, energy, u)


def swap(x, axes):
    return lax.all_to_all(x, axes, split_axis=0, concat_axis=0, tiled=True)


def per_device(field_in, ln_gain, ln_shift, mix_first, mix_bias, mix_second):
    _, band_rows, lon_cells = field_in.shape
    lat_parts = lax.axis_size(LAT)
    lat_rows = band_rows * lat_parts
    tf, ti, tl = (jnp.asarray(t) for t in host_tables())
    tw = tl.reshape(2, lat_parts, 24, lon_cells).transpose(1, 0, 2, 3).reshape(768, lon_cells)
    row_pos = (lax.axis_index(LAT) * band_rows + jnp.arange(band_rows)).astype(F32)
    area = jnp.cos((row_pos + 0.5) * (math.pi / lat_rows) - 0.5 * math.pi)[:, None]
    bias = mix_bias.astype(F32).reshape(mix_bias.shape[0], 2, -1)
    layers = mix_first.shape[0]
    current, stats = field_in, first_stats(field_in)
    band = pay = None
    for layer in range(layers):
        stats = swap(stats, CH)
        if layer == 0:
            normed, lon, band = norm_lon(layer, ln_gain, ln_shift, current, tw, stats, area)
        else:
            sums, pay = band_sums(stats, area, band)
            pay = swap(pay, LAT)
            normed, lon = norm_lon(layer, ln_gain, ln_shift, current, tw, sums, pay)
        back = spectral(layer, swap(lon, LAT), mix_first, bias, mix_second, tf, ti)
        first, last = layer == 0, layer == layers - 1
        extra = ([] if first else [pay]) + ([area] if last else [])
        current, stats = spatial(first, last, extra, swap(back, LAT), current, normed, tl)
    return final_scale(pay, swap(stats, LAT_CH), current)


def solution(mesh):
    finer = Mesh(mesh.devices.reshape(4, 4, 4, 2), LAT_CH)
    in_specs = (
        P(CH, LAT, None),
        P(None, CH),
        P(None, CH),
        P(None, None, CH, None, None),
        P(None, None, CH, None),
        P(None, None, CH, None, None),
    )
    return jax.shard_map(
        per_device, mesh=finer, in_specs=in_specs, out_specs=P(CH, LAT, None), check_vma=False
    )
```

```python
import math

import jax
import jax.numpy as jnp
import numpy as np
from jax import lax
from jax.experimental import pallas as pl
from jax.experimental.pallas import tpu as pltpu
from jax.sharding import Mesh
from jax.sharding import PartitionSpec as P

CH = ("ch_0", "ch_1")
LAT = ("lat_0", "lat_1")
LAT_CH = LAT + CH
NORM_EPS = 1e-05
CH_ALL = 768
GROUPS = 6
MIX_STEP = 8
NORM_MIB, SPECTRAL_MIB, SPATIAL_MIB = 12, 24, 12
F32, BF16 = jnp.float32, jnp.bfloat16
VM = pl.BlockSpec(memory_space=pltpu.VMEM)
SM = pl.BlockSpec(memory_space=pltpu.SMEM)


def host_tables():
    def trig(length, freqs):
        n = np.arange(length)
        a = (n[:, None] * freqs[None, :] % length) * (2.0*math.pi/length)
        s = 1.0/math.sqrt(length)
        bf = jnp.bfloat16
        return (np.cos(a)*s).astype(bf), (np.sin(a)*s).astype(bf)
    c, s = trig(384, np.arange(384))
    tf = np.concatenate([c, s], 1)
    re = np.concatenate([c.T, -s.T], 1).reshape(16, 24, 768)
    im = np.concatenate([s.T, c.T], 1).reshape(16, 24, 768)
    ti = np.stack([re, im], 1).reshape(768, 768)
    lc, ls = trig(768, np.arange(384))
    t = np.concatenate([lc.T, -ls.T], 0)
    return tf, ti, t


def lanes_of(g):
    return pl.ds(pl.multiple_of(g * 384, 384), 384)


def chans_of(g):
    return pl.ds(pl.multiple_of(g * 16, 16), 16)


def exchange_into(xs, unit, put):
    for c in range(len(xs)):
        put(c, jnp.concatenate([x[:, unit * c : unit * (c + 1)] for x in xs], axis=1))


def dot(a, b, dims=((1,), (0,))):
    return lax.dot_general(a, b, (dims, ((), ())), preferred_element_type=F32)


def params(mib):
    return pltpu.CompilerParams(vmem_limit_bytes=mib << 20)


def cost(flops, moved):
    return pl.CostEstimate(flops=flops, bytes_accessed=moved, transcendentals=0)


def put_stats(st_ref, sums, squares):
    for dest in range(st_ref.shape[0]):
        st_ref[dest, 0] = sums.astype(BF16)
        st_ref[dest, 1] = squares.astype(BF16)


def first_stats_kernel(v_ref, st_ref, sum_ref, sq_ref):
    sum_ref[...] = jnp.zeros_like(sum_ref)
    sq_ref[...] = jnp.zeros_like(sq_ref)

    def group(g, _):
        v = v_ref[chans_of(g)].astype(F32)
        sum_ref[...] += jnp.sum(v, axis=0)
        sq_ref[...] += jnp.sum(v * v, axis=0)
        return 0

    lax.fori_loop(0, GROUPS, group, 0)
    put_stats(st_ref, sum_ref[...], sq_ref[...])


def first_stats(v):
    plane = v.shape[1:]
    return pl.pallas_call(
        first_stats_kernel,
        out_shape=jax.ShapeDtypeStruct((8, 2, *plane), BF16),
        in_specs=[VM],
        out_specs=VM,
        scratch_shapes=[pltpu.VMEM(plane, F32), pltpu.VMEM(plane, F32)],
        compiler_params=params(8),
        cost_estimate=cost(6 * 10**6, 4 * 10**6),
        name="first_stats",
    )(v)


def gather_stats(st_ref):
    return tuple(sum(st_ref[d, i].astype(F32) for d in range(st_ref.shape[0])) for i in range(2))


def band_energy(squares):
    rows = squares.shape[0]
    first_row = lax.axis_index(LAT) * rows
    row_pos = (first_row + lax.broadcasted_iota(jnp.int32, squares.shape, 0)).astype(F32)
    area = jnp.cos((row_pos + 0.5) * (math.pi / (rows * lax.axis_size(LAT))) - 0.5 * math.pi)
    return jnp.sum(area * squares, keepdims=True)


def band_kernel(st_ref, first_ref, sums_ref, pay_ref):
    total, squares = gather_stats(st_ref)
    sums_ref[0] = total
    sums_ref[1] = squares
    here = jnp.broadcast_to(band_energy(squares), (1, 128))
    for dest in range(pay_ref.shape[0]):
        pay_ref[dest, 0:1] = first_ref[...]
        pay_ref[dest, 1:2] = here


def band_sums(stats, first):
    plane = stats.shape[2:]
    return pl.pallas_call(
        band_kernel,
        out_shape=(jax.ShapeDtypeStruct((2, *plane), F32), jax.ShapeDtypeStruct((16, 2, 128), F32)),
        in_specs=[VM] * 2,
        out_specs=(VM, VM),
        compiler_params=params(8),
        cost_estimate=cost(10**6, 10**6),
        name="band_sums",
    )(stats, first)


def layer_scale(pay_ref):
    both = jnp.sum(pay_ref[...], axis=0)
    return jnp.sqrt(both[0:1] / both[1:2])[0, 0]


def norm_kernel(layer, gain_ref, shift_ref, v_ref, tw_ref, *refs):
    if layer == 0:
        st_ref, n_ref, o_ref, band_ref, mean_ref, inv_ref = refs
        scale = 1.0
        total, squares = gather_stats(st_ref)
        band_ref[...] = jnp.broadcast_to(band_energy(squares), (1, 128))
    else:
        sums_ref, pay_ref, n_ref, o_ref, mean_ref, inv_ref = refs
        scale = layer_scale(pay_ref)
        total, squares = sums_ref[0], sums_ref[1]
    mean = total / CH_ALL
    spread = squares / CH_ALL - mean * mean
    mean_ref[...] = mean
    inv_ref[...] = scale * lax.rsqrt(spread * (scale * scale) + NORM_EPS)

    def group(g, _):
        mean, inv = mean_ref[...], inv_ref[...]
        rows = []
        for i in range(16):
            c = g * 16 + i
            rows.append((v_ref[c].astype(F32) - mean) * inv * gain_ref[layer, c] + shift_ref[layer, c])
        x = jnp.concatenate(rows, axis=0).astype(BF16)
        n_ref[chans_of(g)] = x.astype(F32).reshape(16, 24, 768).astype(BF16)
        out = dot(tw_ref[...], x, ((1,), (1,)))
        o_ref[:, :, lanes_of(g)] = out.astype(BF16).reshape(16, 48, 384)
        return 0

    lax.fori_loop(0, GROUPS, group, 0, unroll=2)


def norm_lon(layer, gain, shift, v, tw, *stats):
    plane = v.shape[1:]
    outs = [jax.ShapeDtypeStruct(v.shape, BF16), jax.ShapeDtypeStruct((16, 48, 2304), BF16)]
    if layer == 0:
        outs.append(jax.ShapeDtypeStruct((1, 128), F32))

    def kernel(*refs):
        norm_kernel(layer, *refs)

    return pl.pallas_call(
        kernel,
        out_shape=tuple(outs),
        in_specs=[SM, SM] + [VM] * (2 + len(stats)),
        out_specs=(VM,) * len(outs),
        scratch_shapes=[pltpu.VMEM(plane, F32), pltpu.VMEM(plane, F32)],
        compiler_params=params(NORM_MIB),
        cost_estimate=cost(3 * 10**9, 10**7),
        name="norm_lon",
    )(gain, shift, v, tw, *stats)


def complex_weight(w_ref, layer):
    re, im = (w_ref[layer, part, 0].astype(F32).T for part in range(2))
    rows = [jnp.concatenate([re, -im], axis=1), jnp.concatenate([im, re], axis=1)]
    return jnp.concatenate(rows, axis=0).astype(BF16)


def spectral_kernel(layer, r_ref, wa_ref, ba_ref, wb_ref, tf_ref, ti_ref, o_ref, g_ref, f_ref, h_ref):
    def forward(g, _):
        l = lanes_of(g)
        for t in range(3):

            def put(c, v, t=t):
                g_ref[48 * c + 16 * t : 48 * c + 16 * t + 16, :] = v

            exchange_into([r_ref[p, 16 * t : 16 * t + 16, l] for p in range(16)], 24, put)
        prod = dot(g_ref[...], tf_ref[...]).reshape(16, 48, 768)
        re, im = prod[:, :24], prod[:, 24:]
        for k in range(3):
            a, b = slice(128 * k, 128 * k + 128), slice(384 + 128 * k, 512 + 128 * k)
            f_ref[k, l, :] = (re[:, :, a] + im[:, :, b]).reshape(384, 128)
            f_ref[3 + k, l, :] = (im[:, :, a] - re[:, :, b]).reshape(384, 128)
        return 0

    lax.fori_loop(0, GROUPS, forward, 0, unroll=3)
    w1, w2 = complex_weight(wa_ref, layer), complex_weight(wb_ref, layer)
    b1 = jnp.concatenate([ba_ref[layer, part].T for part in range(2)], axis=0)

    def mix(i, _):
        rows = [pl.ds(i * MIX_STEP + k, 96, stride=24) for k in range(MIX_STEP)]
        s = jnp.concatenate(
            [
                jnp.concatenate([f_ref[3 * part + k, row, :].astype(BF16) for row in rows for k in range(3)], axis=1)
                for part in range(2)
            ],
            axis=0,
        )
        hid = jnp.maximum(dot(w1, s) + b1, 0.0).astype(BF16)
        out = dot(w2, hid)
        out = jnp.where(out > 0.01, out - 0.01, jnp.where(out < -0.01, out + 0.01, 0.0))
        for n, row in enumerate(rows):
            for part in range(2):
                for k in range(3):
                    lane = 384 * n + 128 * k
                    h_ref[3 * part + k, row, :] = out[96 * part : 96 * part + 96, lane : lane + 128]
        return 0

    lax.fori_loop(0, 24 // MIX_STEP, mix, 0)

    def inverse(g, _):
        l = lanes_of(g)
        hb = jnp.concatenate([h_ref[k, l, :].astype(BF16) for k in range(6)], axis=1)
        out = dot(ti_ref[...], hb, ((1,), (1,)))
        o_ref[:, :, l] = out.astype(BF16).reshape(16, 48, 384)
        return 0

    lax.fori_loop(0, GROUPS, inverse, 0, unroll=3)


def spectral(layer, r, wa, ba, wb, tf, ti):
    def kernel(*refs):
        spectral_kernel(layer, *refs)

    return pl.pallas_call(
        kernel,
        out_shape=jax.ShapeDtypeStruct(r.shape, BF16),
        in_specs=[VM] * 6,
        out_specs=VM,
        scratch_shapes=[
            pltpu.VMEM((768, 384), BF16),
            pltpu.VMEM((6, 2304, 128), F32),
            pltpu.VMEM((6, 2304, 128), F32),
        ],
        compiler_params=params(SPECTRAL_MIB),
        cost_estimate=cost(12 * 10**9, 10**7),
        name="spectral",
    )(r, wa, ba, wb, tf, ti)


def spatial_kernel(first, last, *refs):
    refs = list(refs)
    scale = 1.0 if first else layer_scale(refs.pop(0))
    y_ref, v_ref, n_ref, tl_ref, u_ref, st_ref, z_ref, sum_ref, sq_ref = refs
    mask = jnp.where(lax.broadcasted_iota(jnp.int32, (1, 384), 1) == 0, 1.0, 2.0)
    sum_ref[...] = jnp.zeros_like(sum_ref)
    sq_ref[...] = jnp.zeros_like(sq_ref)

    def inverse(g, _):
        l = lanes_of(g)
        for t in range(3):

            def put(c, v, t=t):
                z_ref[48 * c + 16 * t : 48 * c + 16 * t + 16, :] = v.astype(F32) * mask

            exchange_into([y_ref[p, 16 * t : 16 * t + 16, l] for p in range(16)], 24, put)
        z = z_ref[...].reshape(16, 48, 384)
        lhs = jnp.concatenate([z[:, :24], z[:, 24:]], axis=2).reshape(384, 768).astype(BF16)
        sp = dot(lhs, tl_ref[...]).reshape(16, 24, 768)
        d = chans_of(g)
        u = sp + n_ref[d].astype(F32) + v_ref[d].astype(F32) * scale
        u_ref[d] = u.astype(BF16)
        sum_ref[...] += jnp.sum(u, axis=0)
        sq_ref[...] += jnp.sum(u * u, axis=0)
        return 0

    lax.fori_loop(0, GROUPS, inverse, 0, unroll=2)
    if last:
        st_ref[...] = jnp.broadcast_to(band_energy(sq_ref[...]).reshape(1, 1, 1), st_ref.shape)
    else:
        put_stats(st_ref, sum_ref[...], sq_ref[...])


def spatial(first, last, extra, y, v, n, tl):
    plane = v.shape[1:]
    stats = jax.ShapeDtypeStruct((128, 1, 128), F32) if last else jax.ShapeDtypeStruct((8, 2, *plane), BF16)

    def kernel(*refs):
        spatial_kernel(first, last, *refs)

    return pl.pallas_call(
        kernel,
        out_shape=(jax.ShapeDtypeStruct(v.shape, BF16), stats),
        in_specs=[VM] * (len(extra) + 4),
        out_specs=(VM, VM),
        scratch_shapes=[pltpu.VMEM((768, 384), F32), pltpu.VMEM(plane, F32), pltpu.VMEM(plane, F32)],
        compiler_params=params(SPATIAL_MIB),
        cost_estimate=cost(3 * 10**9, 15 * 10**6),
        name="spatial",
    )(*extra, y, v, n, tl)


def final_kernel(pay_ref, energy_ref, u_ref, o_ref):
    target = jnp.sum(pay_ref[...], axis=0)[0:1]
    energy = jnp.sum(energy_ref[...], axis=0)
    scale = jnp.sqrt(target / energy)[0, 0]
    d = pl.ds(pl.program_id(0) * o_ref.shape[0], o_ref.shape[0])
    o_ref[...] = (u_ref[d].astype(F32) * scale).astype(BF16)


def final_scale(pay, energy, u):
    return pl.pallas_call(
        final_kernel,
        out_shape=jax.ShapeDtypeStruct(u.shape, BF16),
        grid=(6,),
        in_specs=[VM] * 3,
        out_specs=pl.BlockSpec((16, *u.shape[1:]), lambda g: (g, 0, 0)),
        compiler_params=params(8),
        cost_estimate=cost(10**7, 7 * 10**6),
        name="final_scale",
    )(pay, energy, u)


def swap(x, axes):
    return lax.all_to_all(x, axes, split_axis=0, concat_axis=0, tiled=True)


def per_device(field_in, ln_gain, ln_shift, mix_first, mix_bias, mix_second):
    lon_cells = field_in.shape[-1]
    lat_parts = lax.axis_size(LAT)
    tf, ti, tl = (jnp.asarray(t) for t in host_tables())
    tw = tl.reshape(2, lat_parts, 24, lon_cells).transpose(1, 0, 2, 3).reshape(768, lon_cells)
    layers = mix_first.shape[0]
    current = field_in
    stats, bias = lax.optimization_barrier((first_stats(field_in), mix_bias.astype(F32)))
    band = pay = None
    for layer in range(layers):
        stats = swap(stats, CH)
        if layer == 0:
            normed, lon, band = norm_lon(layer, ln_gain, ln_shift, current, tw, stats)
        else:
            sums, pay = band_sums(stats, band)
            pay = swap(pay, LAT)
            normed, lon = norm_lon(layer, ln_gain, ln_shift, current, tw, sums, pay)
        back = spectral(layer, swap(lon, LAT), mix_first, bias, mix_second, tf, ti)
        first, last = layer == 0, layer == layers - 1
        extra = [] if first else [pay]
        current, stats = spatial(first, last, extra, swap(back, LAT), current, normed, tl)
    return final_scale(pay, swap(stats, LAT_CH), current)


def solution(mesh):
    finer = Mesh(mesh.devices.reshape(4, 4, 4, 2), LAT_CH)
    in_specs = (
        P(CH, LAT, None),
        P(None, CH),
        P(None, CH),
        P(None, None, CH, None, None),
        P(None, None, CH, None),
        P(None, None, CH, None, None),
    )
    return jax.shard_map(
        per_device, mesh=finer, in_specs=in_specs, out_specs=P(CH, LAT, None), check_vma=False
    )
```

```python
import math

import jax
import jax.numpy as jnp
import numpy as np
from jax import lax
from jax.experimental import pallas as pl
from jax.experimental.pallas import tpu as pltpu
from jax.sharding import Mesh
from jax.sharding import PartitionSpec as P

CH = ("ch_0", "ch_1")
LAT = ("lat_0", "lat_1")
LAT_CH = LAT + CH
NORM_EPS = 1e-05
CH_ALL = 768
GROUPS = 6
MIX_STEP = 8
NORM_MIB, SPECTRAL_MIB, SPATIAL_MIB = 12, 24, 12
F32, BF16 = jnp.float32, jnp.bfloat16
VM = pl.BlockSpec(memory_space=pltpu.VMEM)
SM = pl.BlockSpec(memory_space=pltpu.SMEM)


def host_tables():
    def trig(length, freqs):
        n = np.arange(length)
        a = (n[:, None] * freqs[None, :] % length) * (2.0*math.pi/length)
        s = 1.0/math.sqrt(length)
        bf = jnp.bfloat16
        return (np.cos(a)*s).astype(bf), (np.sin(a)*s).astype(bf)
    c, s = trig(384, np.arange(384))
    tf = np.concatenate([c, s], 1)
    re = np.concatenate([c.T, -s.T], 1).reshape(16, 24, 768)
    im = np.concatenate([s.T, c.T], 1).reshape(16, 24, 768)
    ti = np.stack([re, im], 1).reshape(768, 768)
    lc, ls = trig(768, np.arange(384))
    t = np.concatenate([lc.T, -ls.T], 0)
    return tf, ti, t


def lanes_of(g):
    return pl.ds(pl.multiple_of(g * 384, 384), 384)


def chans_of(g):
    return pl.ds(pl.multiple_of(g * 16, 16), 16)


def exchange_into(xs, unit, put):
    for c in range(len(xs)):
        put(c, jnp.concatenate([x[:, unit * c : unit * (c + 1)] for x in xs], axis=1))


def dot(a, b, dims=((1,), (0,))):
    return lax.dot_general(a, b, (dims, ((), ())), preferred_element_type=F32)


def params(mib):
    return pltpu.CompilerParams(vmem_limit_bytes=mib << 20)


def cost(flops, moved):
    return pl.CostEstimate(flops=flops, bytes_accessed=moved, transcendentals=0)


def put_stats(st_ref, sums, squares):
    st_ref[0] = sums.astype(BF16)
    st_ref[1] = squares.astype(BF16)


def band_energy(squares):
    rows = squares.shape[0]
    first_row = lax.axis_index(LAT) * rows
    row_pos = (first_row + lax.broadcasted_iota(jnp.int32, squares.shape, 0)).astype(F32)
    area = jnp.cos((row_pos + 0.5) * (math.pi / (rows * lax.axis_size(LAT))) - 0.5 * math.pi)
    return jnp.sum(area * squares, keepdims=True)


def first_stats_kernel(v_ref, st_ref, sum_ref, sq_ref):
    sum_ref[...] = jnp.zeros_like(sum_ref)
    sq_ref[...] = jnp.zeros_like(sq_ref)

    def group(g, _):
        v = v_ref[chans_of(g)].astype(F32)
        sum_ref[...] += jnp.sum(v, axis=0)
        sq_ref[...] += jnp.sum(v * v, axis=0)
        return 0

    lax.fori_loop(0, GROUPS, group, 0)
    put_stats(st_ref, sum_ref[...], sq_ref[...])


def first_stats(v):
    plane = v.shape[1:]
    return pl.pallas_call(
        first_stats_kernel,
        out_shape=jax.ShapeDtypeStruct((2, *plane), BF16),
        in_specs=[VM],
        out_specs=VM,
        scratch_shapes=[pltpu.VMEM(plane, F32), pltpu.VMEM(plane, F32)],
        compiler_params=params(8),
        cost_estimate=cost(6 * 10**6, 4 * 10**6),
        name="first_stats",
    )(v)


def gather_stats(st_refs):
    return tuple(sum(st_ref[i].astype(F32) for st_ref in st_refs) for i in range(2))


def band_kernel(first_ref, *refs):
    *st_refs, sums_ref, pay_ref = refs
    total, squares = gather_stats(st_refs)
    sums_ref[0] = total
    sums_ref[1] = squares
    both = jnp.concatenate([first_ref[...], jnp.broadcast_to(band_energy(squares), (1, 128))], axis=0)
    pay_ref[...] = jnp.broadcast_to(both[None], pay_ref.shape)


def band_sums(first, parts):
    return pl.pallas_call(
        band_kernel,
        out_shape=(jax.ShapeDtypeStruct(parts[0].shape, F32), jax.ShapeDtypeStruct((16, 2, 128), F32)),
        in_specs=[VM] * (1 + len(parts)),
        out_specs=(VM, VM),
        compiler_params=params(8),
        cost_estimate=cost(10**6, 10**6),
        name="band_sums",
    )(first, *parts)


def layer_scale(pay_ref):
    both = jnp.sum(pay_ref[...], axis=0)
    return jnp.sqrt(both[0:1] / both[1:2])[0, 0]


def norm_kernel(layer, gain_ref, shift_ref, v_ref, tw_ref, *refs):
    if layer == 0:
        *st_refs, n_ref, o_ref, band_ref, mean_ref, inv_ref = refs
        scale = 1.0
        total, squares = gather_stats(st_refs)
        band_ref[...] = jnp.broadcast_to(band_energy(squares), (1, 128))
    else:
        pay_ref, sums_ref, n_ref, o_ref, mean_ref, inv_ref = refs
        scale = layer_scale(pay_ref)
        total, squares = sums_ref[0], sums_ref[1]
    mean = total / CH_ALL
    spread = squares / CH_ALL - mean * mean
    mean_ref[...] = mean
    inv_ref[...] = scale * lax.rsqrt(spread * (scale * scale) + NORM_EPS)

    def group(g, _):
        mean, inv = mean_ref[...], inv_ref[...]
        rows = []
        for i in range(16):
            c = g * 16 + i
            rows.append((v_ref[c].astype(F32) - mean) * inv * gain_ref[layer, c] + shift_ref[layer, c])
        x = jnp.concatenate(rows, axis=0).astype(BF16)
        n_ref[chans_of(g)] = x.astype(F32).reshape(16, 24, 768).astype(BF16)
        out = dot(tw_ref[...], x, ((1,), (1,)))
        o_ref[:, :, lanes_of(g)] = out.astype(BF16).reshape(16, 48, 384)
        return 0

    lax.fori_loop(0, GROUPS, group, 0, unroll=2)


def norm_lon(layer, gain, shift, v, tw, *stats):
    plane = v.shape[1:]
    outs = [jax.ShapeDtypeStruct(v.shape, BF16), jax.ShapeDtypeStruct((16, 48, 2304), BF16)]

    if layer == 0:
        outs.append(jax.ShapeDtypeStruct((1, 128), F32))

    def kernel(*refs):
        norm_kernel(layer, *refs)

    return pl.pallas_call(
        kernel,
        out_shape=tuple(outs),
        in_specs=[SM, SM] + [VM] * (2 + len(stats)),
        out_specs=(VM,) * len(outs),
        scratch_shapes=[pltpu.VMEM(plane, F32), pltpu.VMEM(plane, F32)],
        compiler_params=params(NORM_MIB),
        cost_estimate=cost(3 * 10**9, 10**7),
        name="norm_lon",
    )(gain, shift, v, tw, *stats)


def complex_weight(w_ref, layer):
    re, im = (w_ref[layer, part, 0].astype(F32).T for part in range(2))
    rows = [jnp.concatenate([re, -im], axis=1), jnp.concatenate([im, re], axis=1)]
    return jnp.concatenate(rows, axis=0).astype(BF16)


def spectral_kernel(layer, r_ref, wa_ref, ba_ref, wb_ref, tf_ref, ti_ref, o_ref, g_ref, f_ref, h_ref):
    def forward(g, _):
        l = lanes_of(g)
        for t in range(3):

            def put(c, v, t=t):
                g_ref[48 * c + 16 * t : 48 * c + 16 * t + 16, :] = v

            exchange_into([r_ref[p, 16 * t : 16 * t + 16, l] for p in range(16)], 24, put)
        prod = dot(g_ref[...], tf_ref[...]).reshape(16, 48, 768)
        re, im = prod[:, :24], prod[:, 24:]
        for k in range(3):
            a, b = slice(128 * k, 128 * k + 128), slice(384 + 128 * k, 512 + 128 * k)
            f_ref[k, l, :] = (re[:, :, a] + im[:, :, b]).reshape(384, 128)
            f_ref[3 + k, l, :] = (im[:, :, a] - re[:, :, b]).reshape(384, 128)
        return 0

    lax.fori_loop(0, GROUPS, forward, 0, unroll=3)
    w1, w2 = complex_weight(wa_ref, layer), complex_weight(wb_ref, layer)
    b1 = jnp.concatenate([ba_ref[layer, part : part + 1].astype(F32).T for part in range(2)], axis=0)

    def mix(i, _):
        rows = [pl.ds(i * MIX_STEP + k, 96, stride=24) for k in range(MIX_STEP)]
        s = jnp.concatenate(
            [
                jnp.concatenate([f_ref[3 * part + k, row, :].astype(BF16) for row in rows for k in range(3)], axis=1)
                for part in range(2)
            ],
            axis=0,
        )
        hid = jnp.maximum(dot(w1, s) + b1, 0.0).astype(BF16)
        out = dot(w2, hid)
        out = jnp.where(out > 0.01, out - 0.01, jnp.where(out < -0.01, out + 0.01, 0.0))
        for n, row in enumerate(rows):
            for part in range(2):
                for k in range(3):
                    lane = 384 * n + 128 * k
                    h_ref[3 * part + k, row, :] = out[96 * part : 96 * part + 96, lane : lane + 128]
        return 0

    lax.fori_loop(0, 24 // MIX_STEP, mix, 0)

    def inverse(g, _):
        l = lanes_of(g)
        hb = jnp.concatenate([h_ref[k, l, :].astype(BF16) for k in range(6)], axis=1)
        out = dot(ti_ref[...], hb, ((1,), (1,)))
        o_ref[:, :, l] = out.astype(BF16).reshape(16, 48, 384)
        return 0

    lax.fori_loop(0, GROUPS, inverse, 0, unroll=3)


def spectral(layer, r, wa, ba, wb, tf, ti):
    def kernel(*refs):
        spectral_kernel(layer, *refs)

    return pl.pallas_call(
        kernel,
        out_shape=jax.ShapeDtypeStruct(r.shape, BF16),
        in_specs=[VM] * 6,
        out_specs=VM,
        scratch_shapes=[
            pltpu.VMEM((768, 384), BF16),
            pltpu.VMEM((6, 2304, 128), F32),
            pltpu.VMEM((6, 2304, 128), F32),
        ],
        compiler_params=params(SPECTRAL_MIB),
        cost_estimate=cost(12 * 10**9, 10**7),
        name="spectral",
    )(r, wa, ba, wb, tf, ti)


def spatial_kernel(first, last, *refs):
    refs = list(refs)
    scale = 1.0 if first else layer_scale(refs.pop(0))
    y_ref, v_ref, n_ref, tl_ref, u_ref, st_ref, z_ref, sum_ref, sq_ref = refs
    mask = jnp.where(lax.broadcasted_iota(jnp.int32, (1, 384), 1) == 0, 1.0, 2.0)
    sum_ref[...] = jnp.zeros_like(sum_ref)
    sq_ref[...] = jnp.zeros_like(sq_ref)

    def inverse(g, _):
        l = lanes_of(g)
        for t in range(3):

            def put(c, v, t=t):
                z_ref[48 * c + 16 * t : 48 * c + 16 * t + 16, :] = v.astype(F32) * mask

            exchange_into([y_ref[p, 16 * t : 16 * t + 16, l] for p in range(16)], 24, put)
        z = z_ref[...].reshape(16, 48, 384)
        lhs = jnp.concatenate([z[:, :24], z[:, 24:]], axis=2).reshape(384, 768).astype(BF16)
        sp = dot(lhs, tl_ref[...]).reshape(16, 24, 768)
        d = chans_of(g)
        u = sp + n_ref[d].astype(F32) + v_ref[d].astype(F32) * scale
        u_ref[d] = u.astype(BF16)
        sum_ref[...] += jnp.sum(u, axis=0)
        sq_ref[...] += jnp.sum(u * u, axis=0)
        return 0

    lax.fori_loop(0, GROUPS, inverse, 0, unroll=2)
    if last:
        st_ref[...] = jnp.broadcast_to(band_energy(sq_ref[...]).reshape(1, 1, 1), st_ref.shape)
    else:
        put_stats(st_ref, sum_ref[...], sq_ref[...])


def spatial(first, last, extra, y, v, n, tl):
    plane = v.shape[1:]
    stats = jax.ShapeDtypeStruct((128, 1, 128), F32) if last else jax.ShapeDtypeStruct((2, *plane), BF16)

    def kernel(*refs):
        spatial_kernel(first, last, *refs)

    return pl.pallas_call(
        kernel,
        out_shape=(jax.ShapeDtypeStruct(v.shape, BF16), stats),
        in_specs=[VM] * (len(extra) + 4),
        out_specs=(VM, VM),
        scratch_shapes=[pltpu.VMEM((768, 384), F32), pltpu.VMEM(plane, F32), pltpu.VMEM(plane, F32)],
        compiler_params=params(SPATIAL_MIB),
        cost_estimate=cost(3 * 10**9, 15 * 10**6),
        name="spatial",
    )(*extra, y, v, n, tl)


def final_kernel(pay_ref, energy_ref, u_ref, o_hbm, o_ref, sems):
    def store(g):
        return pltpu.make_async_copy(o_ref.at[chans_of(g)], o_hbm.at[chans_of(g)], sems.at[g])

    target = jnp.sum(pay_ref[...], axis=0)[0:1]
    energy = jnp.sum(energy_ref[...], axis=0)
    scale = jnp.sqrt(target / energy)[0, 0]

    def group(g, _):
        o_ref[chans_of(g)] = (u_ref[chans_of(g)].astype(F32) * scale).astype(BF16)
        store(g).start()
        return 0

    lax.fori_loop(0, GROUPS, group, 0)

    def drain(g, _):
        store(g).wait()
        return 0

    lax.fori_loop(0, GROUPS, drain, 0)


def final_scale(pay, energy, u):
    return pl.pallas_call(
        final_kernel,
        out_shape=jax.ShapeDtypeStruct(u.shape, BF16),
        in_specs=[VM] * 3,
        out_specs=pl.BlockSpec(memory_space=pl.ANY),
        scratch_shapes=[pltpu.VMEM(u.shape, BF16), pltpu.SemaphoreType.DMA((GROUPS,))],
        compiler_params=params(12),
        cost_estimate=cost(10**7, 7 * 10**6),
        name="final_scale",
    )(pay, energy, u)


def swap(x, axes):
    return lax.all_to_all(x, axes, split_axis=0, concat_axis=0, tiled=True)


def ring(x, axis, step):
    n = lax.axis_size(axis)
    return lax.ppermute(x, axis, [(i, (i + step) % n) for i in range(n)])


def stat_parts(stats):
    pair = (stats.astype(F32) + ring(stats, CH[1], 1).astype(F32)).astype(BF16)
    return [pair] + [ring(pair, CH[0], step) for step in range(1, lax.axis_size(CH[0]))]


def per_device(field_in, ln_gain, ln_shift, mix_first, mix_bias, mix_second):
    lon_cells = field_in.shape[-1]
    lat_parts = lax.axis_size(LAT)
    tf, ti, tl = (jnp.asarray(t) for t in host_tables())
    tw = tl.reshape(2, lat_parts, 24, lon_cells).transpose(1, 0, 2, 3).reshape(768, lon_cells)
    layers = mix_first.shape[0]
    bias = mix_bias.reshape(layers, 2, -1)
    current, stats = field_in, first_stats(field_in)
    band, scales = None, []
    for layer in range(layers):
        parts = stat_parts(stats)
        if layer == 0:
            normed, lon, band = norm_lon(layer, ln_gain, ln_shift, current, tw, *parts)
        else:
            sums, pay = band_sums(band, parts)
            scales = [swap(pay, LAT)]
            normed, lon = norm_lon(layer, ln_gain, ln_shift, current, tw, *scales, sums)
        back = spectral(layer, swap(lon, LAT), mix_first, bias, mix_second, tf, ti)
        first, last = layer == 0, layer == layers - 1
        current, stats = spatial(first, last, scales, swap(back, LAT), current, normed, tl)
    return final_scale(scales[0], swap(stats, LAT_CH), current)


def solution(mesh):
    finer = Mesh(mesh.devices.reshape(4, 4, 4, 2), LAT_CH)
    in_specs = (
        P(CH, LAT, None),
        P(None, CH),
        P(None, CH),
        P(None, None, CH, None, None),
        P(None, None, CH, None),
        P(None, None, CH, None, None),
    )
    return jax.shard_map(
        per_device, mesh=finer, in_specs=in_specs, out_specs=P(CH, LAT, None), check_vma=False
    )
```

```python
import math

import jax
import jax.numpy as jnp
import numpy as np
from jax import lax
from jax.experimental import pallas as pl
from jax.experimental.pallas import tpu as pltpu
from jax.sharding import Mesh
from jax.sharding import PartitionSpec as P

CH = ("ch_0", "ch_1")
LAT = ("lat_0", "lat_1")
LAT_CH = LAT + CH
NORM_EPS = 1e-05
CH_ALL = 768
GROUPS = 6
MIX_STEP = 8
NORM_MIB, SPECTRAL_MIB, SPATIAL_MIB = 12, 24, 12
F32, BF16 = jnp.float32, jnp.bfloat16
VM = pl.BlockSpec(memory_space=pltpu.VMEM)
SM = pl.BlockSpec(memory_space=pltpu.SMEM)


PIECE_ROWS = np.r_[0:16, 24:40, 16:24, 40:48]


def host_tables():
    def trig(length, freqs):
        n = np.arange(length)
        a = (n[:, None] * freqs[None, :] % length) * (2.0 * math.pi / length)
        s = 1.0 / math.sqrt(length)
        return (np.cos(a) * s).astype(jnp.bfloat16), (np.sin(a) * s).astype(jnp.bfloat16)

    def pieces(table):
        return table.reshape(2, 16, 24, 768).transpose(1, 0, 2, 3).reshape(16, 48, 768)[:, PIECE_ROWS].reshape(768, 768)

    c, s = trig(384, np.arange(384))
    lat = np.block([[c, -s], [s, c]])
    c, s = trig(768, np.arange(384))
    lon = np.concatenate([c.T, -s.T], 0)
    twice = np.where(np.arange(768) % 384 == 0, 1.0, 2.0)[:, None]
    weighted = (lon.astype(np.float32) * twice).astype(jnp.bfloat16)
    return lat, pieces(lat), pieces(lon), weighted


def lanes_of(g):
    return pl.ds(pl.multiple_of(g * 384, 384), 384)


def chans_of(g):
    return pl.ds(pl.multiple_of(g * 16, 16), 16)


def exchange(xs, unit):
    n, tile = len(xs), 128
    tiles = n * unit // tile
    lane = lax.broadcasted_iota(jnp.int32, (16, tile), 1).astype(F32).astype(BF16)
    cuts = {k: lane >= jnp.asarray(k, BF16) for k in range(8, tile, 8)}

    def by_block(t, pick):
        out = pick(t * tile // unit)
        for block in range(t * tile // unit + 1, -(-(t + 1) * tile // unit)):
            out = jnp.where(cuts[block * unit - t * tile], pick(block), out)
        return out

    moved = []
    for s in range(n):
        held = [by_block(t, lambda b, t=t: xs[(b + s) % n][:, tile * t : tile * t + tile]) for t in range(tiles)]
        whole, part = divmod(s * unit, tile)
        if part:
            turned = [pltpu.roll(h, part, 1) for h in held]
            moved.append(
                [jnp.where(cuts[part], turned[(t - whole) % tiles], turned[(t - whole - 1) % tiles]) for t in range(tiles)]
            )
        else:
            moved.append([held[(t - whole) % tiles] for t in range(tiles)])
    return [
        jnp.concatenate([by_block(t, lambda b, t=t: moved[(b - c) % n][t]) for t in range(tiles)], axis=1)
        for c in range(n)
    ]


def gather_rows(x_ref, lanes, g_ref):
    for part in range(2):
        cols = slice(384 * part, 384 * part + 384)
        for c, v in enumerate(exchange([x_ref[p, 16 * part : 16 * part + 16, lanes] for p in range(16)], 24)):
            row = 48 * (c // 2) + 16 * (c % 2)
            g_ref[row : row + 16, cols] = v
    tails = exchange([x_ref[p, 32:48, lanes] for p in range(16)], 24)
    for c in range(0, 16, 2):
        row = 24 * c + 32
        for part in range(2):
            half = slice(8 * part, 8 * part + 8)
            g_ref[row : row + 16, 384 * part : 384 * part + 384] = jnp.concatenate(
                [tails[c][half], tails[c + 1][half]], axis=0
            )


def natural_rows(x):
    x = x.reshape(8, 6, 8, 768)
    return jnp.concatenate([x[:, :2], x[:, 4:5], x[:, 2:4], x[:, 5:]], axis=1).reshape(384, 768)


def dot(a, b, dims=((1,), (0,))):
    return lax.dot_general(a, b, (dims, ((), ())), preferred_element_type=F32)


def params(mib):
    return pltpu.CompilerParams(vmem_limit_bytes=mib << 20)


def cost(flops, moved):
    return pl.CostEstimate(flops=flops, bytes_accessed=moved, transcendentals=0)


def put_stats(st_ref, sums, squares):
    st_ref[0] = sums.astype(BF16)
    st_ref[1] = squares.astype(BF16)


def band_energy(squares):
    rows = squares.shape[0]
    first_row = lax.axis_index(LAT) * rows
    row_pos = (first_row + lax.broadcasted_iota(jnp.int32, squares.shape, 0)).astype(F32)
    area = jnp.cos((row_pos + 0.5) * (math.pi / (rows * lax.axis_size(LAT))) - 0.5 * math.pi)
    return jnp.sum(area * squares, keepdims=True)


def first_stats_kernel(v_ref, st_ref, sum_ref, sq_ref):
    sum_ref[...] = jnp.zeros_like(sum_ref)
    sq_ref[...] = jnp.zeros_like(sq_ref)

    def group(g, _):
        v = v_ref[chans_of(g)].astype(F32)
        sum_ref[...] += jnp.sum(v, axis=0)
        sq_ref[...] += jnp.sum(v * v, axis=0)
        return 0

    lax.fori_loop(0, GROUPS, group, 0)
    put_stats(st_ref, sum_ref[...], sq_ref[...])


def first_stats(v):
    plane = v.shape[1:]
    return pl.pallas_call(
        first_stats_kernel,
        out_shape=jax.ShapeDtypeStruct((2, *plane), BF16),
        in_specs=[VM],
        out_specs=VM,
        scratch_shapes=[pltpu.VMEM(plane, F32), pltpu.VMEM(plane, F32)],
        compiler_params=params(8),
        cost_estimate=cost(6 * 10**6, 4 * 10**6),
        name="first_stats",
    )(v)


def gather_stats(st_refs):
    return tuple(sum(st_ref[i].astype(F32) for st_ref in st_refs) for i in range(2))


def band_kernel(first_ref, *refs):
    *st_refs, sums_ref, pay_ref = refs
    total, squares = gather_stats(st_refs)
    sums_ref[0] = total
    sums_ref[1] = squares
    both = jnp.concatenate([first_ref[...], jnp.broadcast_to(band_energy(squares), (1, 128))], axis=0)
    pay_ref[...] = jnp.broadcast_to(both[None], pay_ref.shape)


def band_sums(first, parts):
    return pl.pallas_call(
        band_kernel,
        out_shape=(jax.ShapeDtypeStruct(parts[0].shape, F32), jax.ShapeDtypeStruct((16, 2, 128), F32)),
        in_specs=[VM] * (1 + len(parts)),
        out_specs=(VM, VM),
        compiler_params=params(8),
        cost_estimate=cost(10**6, 10**6),
        name="band_sums",
    )(first, *parts)


def layer_scale(pay_ref):
    both = jnp.sum(pay_ref[...], axis=0)
    return jnp.sqrt(both[0:1] / both[1:2])[0, 0]


def norm_kernel(layer, gain_ref, shift_ref, v_ref, tw_ref, *refs):
    if layer == 0:
        *st_refs, n_ref, o_ref, band_ref, mean_ref, inv_ref = refs
        scale = 1.0
        total, squares = gather_stats(st_refs)
        band_ref[...] = jnp.broadcast_to(band_energy(squares), (1, 128))
    else:
        pay_ref, sums_ref, n_ref, o_ref, mean_ref, inv_ref = refs
        scale = layer_scale(pay_ref)
        total, squares = sums_ref[0], sums_ref[1]
    mean = total / CH_ALL
    spread = squares / CH_ALL - mean * mean
    mean_ref[...] = mean
    inv_ref[...] = scale * lax.rsqrt(spread * (scale * scale) + NORM_EPS)

    def group(g, _):
        mean, inv = mean_ref[...], inv_ref[...]
        rows = []
        for i in range(16):
            c = g * 16 + i
            rows.append((v_ref[c].astype(F32) - mean) * inv * gain_ref[layer, c] + shift_ref[layer, c])
        x = jnp.concatenate(rows, axis=0).astype(BF16)
        n_ref[chans_of(g)] = x.astype(F32).reshape(16, 24, 768).astype(BF16)
        out = dot(tw_ref[...], x, ((1,), (1,)))
        o_ref[:, :, lanes_of(g)] = out.astype(BF16).reshape(16, 48, 384)
        return 0

    lax.fori_loop(0, GROUPS, group, 0, unroll=2)


def norm_lon(layer, gain, shift, v, tw, *stats):
    plane = v.shape[1:]
    outs = [jax.ShapeDtypeStruct(v.shape, BF16), jax.ShapeDtypeStruct((16, 48, 2304), BF16)]

    if layer == 0:
        outs.append(jax.ShapeDtypeStruct((1, 128), F32))

    def kernel(*refs):
        norm_kernel(layer, *refs)

    return pl.pallas_call(
        kernel,
        out_shape=tuple(outs),
        in_specs=[SM, SM] + [VM] * (2 + len(stats)),
        out_specs=(VM,) * len(outs),
        scratch_shapes=[pltpu.VMEM(plane, F32), pltpu.VMEM(plane, F32)],
        compiler_params=params(NORM_MIB),
        cost_estimate=cost(3 * 10**9, 10**7),
        name="norm_lon",
    )(gain, shift, v, tw, *stats)


def complex_weight(w_ref, layer):
    re, im = (w_ref[layer, part, 0].astype(F32).T for part in range(2))
    rows = [jnp.concatenate([re, -im], axis=1), jnp.concatenate([im, re], axis=1)]
    return jnp.concatenate(rows, axis=0).astype(BF16)


def spectral_kernel(layer, r_ref, wa_ref, ba_ref, wb_ref, tf_ref, ti_ref, o_ref, g_ref, f_ref, h_ref):
    def forward(g, _):
        l = lanes_of(g)
        gather_rows(r_ref, l, g_ref)
        prod = natural_rows(dot(g_ref[...], tf_ref[...]))
        for k in range(6):
            f_ref[k, l, :] = prod[:, 128 * k : 128 * k + 128]
        return 0

    lax.fori_loop(0, GROUPS, forward, 0, unroll=6)
    w1, w2 = complex_weight(wa_ref, layer), complex_weight(wb_ref, layer)
    b1 = jnp.concatenate([ba_ref[layer, part : part + 1].astype(F32).T for part in range(2)], axis=0)

    def mix(i, _):
        rows = [pl.ds(i * MIX_STEP + k, 96, stride=24) for k in range(MIX_STEP)]
        s = jnp.concatenate(
            [
                jnp.concatenate([f_ref[3 * part + k, row, :].astype(BF16) for row in rows for k in range(3)], axis=1)
                for part in range(2)
            ],
            axis=0,
        )
        hid = jnp.maximum(dot(w1, s) + b1, 0.0).astype(BF16)
        out = dot(w2, hid)
        out = out - jnp.clip(out, -0.01, 0.01)
        for n, row in enumerate(rows):
            for part in range(2):
                for k in range(3):
                    lane = 384 * n + 128 * k
                    h_ref[3 * part + k, row, :] = out[96 * part : 96 * part + 96, lane : lane + 128]
        return 0

    lax.fori_loop(0, 24 // MIX_STEP, mix, 0)

    def inverse(g, _):
        l = lanes_of(g)
        hb = jnp.concatenate([h_ref[k, l, :].astype(BF16) for k in range(6)], axis=1)
        out = dot(ti_ref[...], hb, ((1,), (1,)))
        o_ref[:, :, l] = out.astype(BF16).reshape(16, 48, 384)
        return 0

    lax.fori_loop(0, GROUPS, inverse, 0, unroll=3)


def spectral(layer, r, wa, ba, wb, tf, ti):
    def kernel(*refs):
        spectral_kernel(layer, *refs)

    return pl.pallas_call(
        kernel,
        out_shape=jax.ShapeDtypeStruct(r.shape, BF16),
        in_specs=[VM] * 6,
        out_specs=VM,
        scratch_shapes=[
            pltpu.VMEM((384, 768), BF16),
            pltpu.VMEM((6, 2304, 128), F32),
            pltpu.VMEM((6, 2304, 128), F32),
        ],
        compiler_params=params(SPECTRAL_MIB),
        cost_estimate=cost(12 * 10**9, 10**7),
        name="spectral",
    )(r, wa, ba, wb, tf, ti)


def spatial_kernel(first, last, *refs):
    refs = list(refs)
    scale = 1.0 if first else layer_scale(refs.pop(0))
    y_ref, v_ref, n_ref, tl_ref, u_ref, st_ref, z_ref, sum_ref, sq_ref = refs
    sum_ref[...] = jnp.zeros_like(sum_ref)
    sq_ref[...] = jnp.zeros_like(sq_ref)

    def inverse(g, _):
        l = lanes_of(g)
        gather_rows(y_ref, l, z_ref)
        sp = natural_rows(dot(z_ref[...], tl_ref[...])).reshape(16, 24, 768)
        d = chans_of(g)
        u = sp + n_ref[d].astype(F32) + v_ref[d].astype(F32) * scale
        u_ref[d] = u.astype(BF16)
        sum_ref[...] += jnp.sum(u, axis=0)
        sq_ref[...] += jnp.sum(u * u, axis=0)
        return 0

    lax.fori_loop(0, GROUPS, inverse, 0, unroll=6)
    if last:
        st_ref[...] = jnp.broadcast_to(band_energy(sq_ref[...]).reshape(1, 1, 1), st_ref.shape)
    else:
        put_stats(st_ref, sum_ref[...], sq_ref[...])


def spatial(first, last, extra, y, v, n, tl):
    plane = v.shape[1:]
    stats = jax.ShapeDtypeStruct((128, 1, 128), F32) if last else jax.ShapeDtypeStruct((2, *plane), BF16)

    def kernel(*refs):
        spatial_kernel(first, last, *refs)

    return pl.pallas_call(
        kernel,
        out_shape=(jax.ShapeDtypeStruct(v.shape, BF16), stats),
        in_specs=[VM] * (len(extra) + 4),
        out_specs=(VM, VM),
        scratch_shapes=[pltpu.VMEM((384, 768), BF16), pltpu.VMEM(plane, F32), pltpu.VMEM(plane, F32)],
        compiler_params=params(SPATIAL_MIB),
        cost_estimate=cost(3 * 10**9, 15 * 10**6),
        name="spatial",
    )(*extra, y, v, n, tl)


def final_kernel(pay_ref, energy_ref, u_ref, o_hbm, o_ref, sems):
    def store(g):
        return pltpu.make_async_copy(o_ref.at[chans_of(g)], o_hbm.at[chans_of(g)], sems.at[g])

    target = jnp.sum(pay_ref[...], axis=0)[0:1]
    energy = jnp.sum(energy_ref[...], axis=0)
    scale = jnp.sqrt(target / energy)[0, 0]

    def group(g, _):
        o_ref[chans_of(g)] = (u_ref[chans_of(g)].astype(F32) * scale).astype(BF16)
        store(g).start()
        return 0

    lax.fori_loop(0, GROUPS, group, 0)

    def drain(g, _):
        store(g).wait()
        return 0

    lax.fori_loop(0, GROUPS, drain, 0)


def final_scale(pay, energy, u):
    return pl.pallas_call(
        final_kernel,
        out_shape=jax.ShapeDtypeStruct(u.shape, BF16),
        in_specs=[VM] * 3,
        out_specs=pl.BlockSpec(memory_space=pl.ANY),
        scratch_shapes=[pltpu.VMEM(u.shape, BF16), pltpu.SemaphoreType.DMA((GROUPS,))],
        compiler_params=params(12),
        cost_estimate=cost(10**7, 7 * 10**6),
        name="final_scale",
    )(pay, energy, u)


def swap(x, axes):
    return lax.all_to_all(x, axes, split_axis=0, concat_axis=0, tiled=True)


def ring(x, axis, step):
    n = lax.axis_size(axis)
    return lax.ppermute(x, axis, [(i, (i + step) % n) for i in range(n)])


def stat_parts(stats):
    pair = (stats.astype(F32) + ring(stats, CH[1], 1).astype(F32)).astype(BF16)
    return [pair] + [ring(pair, CH[0], step) for step in range(1, lax.axis_size(CH[0]))]


def per_device(field_in, ln_gain, ln_shift, mix_first, mix_bias, mix_second):
    tf, ti, tw, tl = (jnp.asarray(t) for t in host_tables())
    layers = mix_first.shape[0]
    bias = mix_bias.reshape(layers, 2, -1)
    current, stats = field_in, first_stats(field_in)
    band, scales = None, []
    for layer in range(layers):
        parts = stat_parts(stats)
        if layer == 0:
            normed, lon, band = norm_lon(layer, ln_gain, ln_shift, current, tw, *parts)
        else:
            sums, pay = band_sums(band, parts)
            scales = [swap(pay, LAT)]
            normed, lon = norm_lon(layer, ln_gain, ln_shift, current, tw, *scales, sums)
        back = spectral(layer, swap(lon, LAT), mix_first, bias, mix_second, tf, ti)
        first, last = layer == 0, layer == layers - 1
        current, stats = spatial(first, last, scales, swap(back, LAT), current, normed, tl)
    return final_scale(scales[0], swap(stats, LAT_CH), current)


def solution(mesh):
    finer = Mesh(mesh.devices.reshape(4, 4, 4, 2), LAT_CH)
    in_specs = (
        P(CH, LAT, None),
        P(None, CH),
        P(None, CH),
        P(None, None, CH, None, None),
        P(None, None, CH, None),
        P(None, None, CH, None, None),
    )
    return jax.shard_map(
        per_device, mesh=finer, in_specs=in_specs, out_specs=P(CH, LAT, None), check_vma=False
    )
```

```python
import math

import jax
import jax.numpy as jnp
import numpy as np
from jax import lax
from jax.experimental import pallas as pl
from jax.experimental.pallas import tpu as pltpu
from jax.sharding import Mesh
from jax.sharding import PartitionSpec as P

CH = ("ch_0", "ch_1")
LAT = ("lat_0", "lat_1")
LAT_CH = LAT + CH
NORM_EPS = 1e-05
CH_ALL = 768
GROUPS = 6
MIX_STEP = 8
NORM_UNROLL = 1
NORM_MIB, SPECTRAL_MIB, SPATIAL_MIB = 12, 24, 12
F32, BF16 = jnp.float32, jnp.bfloat16
VM = pl.BlockSpec(memory_space=pltpu.VMEM)
SM = pl.BlockSpec(memory_space=pltpu.SMEM)


PIECE_ROWS = np.r_[0:16, 24:40, 16:24, 40:48]


def host_tables():
    def trig(length, freqs):
        n = np.arange(length)
        a = (n[:, None] * freqs[None, :] % length) * (2.0 * math.pi / length)
        s = 1.0 / math.sqrt(length)
        return (np.cos(a) * s).astype(jnp.bfloat16), (np.sin(a) * s).astype(jnp.bfloat16)

    def pieces(table):
        return table.reshape(2, 16, 24, 768).transpose(1, 0, 2, 3).reshape(16, 48, 768)[:, PIECE_ROWS].reshape(768, 768)

    c, s = trig(384, np.arange(384))
    lat = np.block([[c, -s], [s, c]])
    c, s = trig(768, np.arange(384))
    lon = np.concatenate([c.T, -s.T], 0)
    twice = np.where(np.arange(768) % 384 == 0, 1.0, 2.0)[:, None]
    weighted = (lon.astype(np.float32) * twice).astype(jnp.bfloat16)
    return lat, pieces(lat), pieces(lon), weighted


def lanes_of(g):
    return pl.ds(pl.multiple_of(g * 384, 384), 384)


def chans_of(g):
    return pl.ds(pl.multiple_of(g * 16, 16), 16)


def exchange(xs, unit):
    n, tile = len(xs), 128
    tiles = n * unit // tile
    lane = lax.broadcasted_iota(jnp.int32, (16, tile), 1).astype(F32).astype(BF16)
    cuts = {k: lane >= jnp.asarray(k, BF16) for k in range(8, tile, 8)}

    def by_block(t, pick):
        out = pick(t * tile // unit)
        for block in range(t * tile // unit + 1, -(-(t + 1) * tile // unit)):
            out = jnp.where(cuts[block * unit - t * tile], pick(block), out)
        return out

    moved = []
    for s in range(n):
        held = [by_block(t, lambda b, t=t: xs[(b + s) % n][:, tile * t : tile * t + tile]) for t in range(tiles)]
        whole, part = divmod(s * unit, tile)
        if part:
            turned = [pltpu.roll(h, part, 1) for h in held]
            moved.append(
                [jnp.where(cuts[part], turned[(t - whole) % tiles], turned[(t - whole - 1) % tiles]) for t in range(tiles)]
            )
        else:
            moved.append([held[(t - whole) % tiles] for t in range(tiles)])
    return [
        jnp.concatenate([by_block(t, lambda b, t=t: moved[(b - c) % n][t]) for t in range(tiles)], axis=1)
        for c in range(n)
    ]


def gather_rows(x_ref, lanes, g_ref):
    for part in range(2):
        cols = slice(384 * part, 384 * part + 384)
        for c, v in enumerate(exchange([x_ref[p, 16 * part : 16 * part + 16, lanes] for p in range(16)], 24)):
            row = 48 * (c // 2) + 16 * (c % 2)
            g_ref[row : row + 16, cols] = v
    tails = exchange([x_ref[p, 32:48, lanes] for p in range(16)], 24)
    for c in range(0, 16, 2):
        row = 24 * c + 32
        for part in range(2):
            half = slice(8 * part, 8 * part + 8)
            g_ref[row : row + 16, 384 * part : 384 * part + 384] = jnp.concatenate(
                [tails[c][half], tails[c + 1][half]], axis=0
            )


def natural_rows(x):
    x = x.reshape(8, 6, 8, 768)
    return jnp.concatenate([x[:, :2], x[:, 4:5], x[:, 2:4], x[:, 5:]], axis=1).reshape(384, 768)


def dot(a, b, dims=((1,), (0,))):
    return lax.dot_general(a, b, (dims, ((), ())), preferred_element_type=F32)


def params(mib):
    return pltpu.CompilerParams(vmem_limit_bytes=mib << 20)


def cost(flops, moved):
    return pl.CostEstimate(flops=flops, bytes_accessed=moved, transcendentals=0)


def put_stats(st_ref, sums, squares):
    st_ref[0] = sums.astype(BF16)
    st_ref[1] = squares.astype(BF16)


def band_energy(squares):
    rows = squares.shape[0]
    first_row = lax.axis_index(LAT) * rows
    row_pos = (first_row + lax.broadcasted_iota(jnp.int32, squares.shape, 0)).astype(F32)
    area = jnp.cos((row_pos + 0.5) * (math.pi / (rows * lax.axis_size(LAT))) - 0.5 * math.pi)
    return jnp.sum(area * squares, keepdims=True)


def first_stats_kernel(v_ref, st_ref, sum_ref, sq_ref):
    sum_ref[...] = jnp.zeros_like(sum_ref)
    sq_ref[...] = jnp.zeros_like(sq_ref)

    def group(g, _):
        v = v_ref[chans_of(g)].astype(F32)
        sum_ref[...] += jnp.sum(v, axis=0)
        sq_ref[...] += jnp.sum(v * v, axis=0)
        return 0

    lax.fori_loop(0, GROUPS, group, 0)
    put_stats(st_ref, sum_ref[...], sq_ref[...])


def first_stats(v):
    plane = v.shape[1:]
    return pl.pallas_call(
        first_stats_kernel,
        out_shape=jax.ShapeDtypeStruct((2, *plane), BF16),
        in_specs=[VM],
        out_specs=VM,
        scratch_shapes=[pltpu.VMEM(plane, F32), pltpu.VMEM(plane, F32)],
        compiler_params=params(8),
        cost_estimate=cost(5 * 10**9, 10**7),
        name="first_stats",
    )(v)


def gather_stats(st_refs):
    return tuple(sum(st_ref[i].astype(F32) for st_ref in st_refs) for i in range(2))


def band_kernel(first_ref, *refs):
    *st_refs, sums_ref, pay_ref = refs
    total, squares = gather_stats(st_refs)
    sums_ref[0] = total
    sums_ref[1] = squares
    both = jnp.concatenate([first_ref[...], jnp.broadcast_to(band_energy(squares), (1, 128))], axis=0)
    pay_ref[...] = jnp.broadcast_to(both[None], pay_ref.shape)


def band_sums(first, parts):
    return pl.pallas_call(
        band_kernel,
        out_shape=(jax.ShapeDtypeStruct(parts[0].shape, F32), jax.ShapeDtypeStruct((16, 2, 128), F32)),
        in_specs=[VM] * (1 + len(parts)),
        out_specs=(VM, VM),
        compiler_params=params(8),
        cost_estimate=cost(10**6, 10**6),
        name="band_sums",
    )(first, *parts)


def layer_scale(pay_ref):
    both = jnp.sum(pay_ref[...], axis=0)
    return jnp.sqrt(both[0:1] / both[1:2])[0, 0]


def norm_kernel(layer, gain_ref, shift_ref, v_ref, tw_ref, *refs):
    if layer == 0:
        *st_refs, n_ref, o_ref, band_ref, mean_ref, inv_ref = refs
        scale = 1.0
        total, squares = gather_stats(st_refs)
        band_ref[...] = jnp.broadcast_to(band_energy(squares), (1, 128))
    else:
        pay_ref, sums_ref, n_ref, o_ref, mean_ref, inv_ref = refs
        scale = layer_scale(pay_ref)
        total, squares = sums_ref[0], sums_ref[1]
    mean = total / CH_ALL
    spread = squares / CH_ALL - mean * mean
    mean_ref[...] = mean
    inv_ref[...] = scale * lax.rsqrt(spread * (scale * scale) + NORM_EPS)

    def group(g, _):
        mean, inv = mean_ref[...], inv_ref[...]
        rows = []
        for i in range(32):
            c = g * 32 + i
            rows.append((v_ref[c].astype(F32) - mean) * inv * gain_ref[layer, c] + shift_ref[layer, c])
        x = jnp.concatenate(rows, axis=0).astype(BF16)
        n_ref[pl.ds(pl.multiple_of(g * 32, 32), 32)] = x.astype(F32).reshape(32, 24, 768).astype(BF16)
        out = dot(tw_ref[...], x, ((1,), (1,)))
        o_ref[:, :, pl.ds(pl.multiple_of(g * 768, 768), 768)] = out.astype(BF16).reshape(16, 48, 768)
        return 0

    lax.fori_loop(0, GROUPS // 2, group, 0, unroll=NORM_UNROLL)


def norm_lon(layer, gain, shift, v, tw, *stats):
    plane = v.shape[1:]
    outs = [jax.ShapeDtypeStruct(v.shape, BF16), jax.ShapeDtypeStruct((16, 48, 2304), BF16)]

    if layer == 0:
        outs.append(jax.ShapeDtypeStruct((1, 128), F32))

    def kernel(*refs):
        norm_kernel(layer, *refs)

    return pl.pallas_call(
        kernel,
        out_shape=tuple(outs),
        in_specs=[SM, SM] + [VM] * (2 + len(stats)),
        out_specs=(VM,) * len(outs),
        scratch_shapes=[pltpu.VMEM(plane, F32), pltpu.VMEM(plane, F32)],
        compiler_params=params(NORM_MIB),
        cost_estimate=cost(3 * 10**9, 10**7),
        name="norm_lon",
    )(gain, shift, v, tw, *stats)


def complex_weight(w_ref, layer):
    re, im = (w_ref[layer, part, 0].astype(F32).T for part in range(2))
    rows = [jnp.concatenate([re, -im], axis=1), jnp.concatenate([im, re], axis=1)]
    return jnp.concatenate(rows, axis=0).astype(BF16)


def spectral_kernel(layer, r_ref, wa_ref, ba_ref, wb_ref, tf_ref, ti_ref, o_ref, g_ref, f_ref, h_ref):
    def forward(g, _):
        l = lanes_of(g)
        gather_rows(r_ref, l, g_ref)
        prod = natural_rows(dot(g_ref[...], tf_ref[...]))
        for k in range(6):
            f_ref[k, l, :] = prod[:, 128 * k : 128 * k + 128]
        return 0

    lax.fori_loop(0, GROUPS, forward, 0, unroll=6)
    w1, w2 = complex_weight(wa_ref, layer), complex_weight(wb_ref, layer)
    b1 = jnp.concatenate([ba_ref[layer, part : part + 1].astype(F32).T for part in range(2)], axis=0)

    def mix(i, _):
        rows = [pl.ds(i * MIX_STEP + k, 96, stride=24) for k in range(MIX_STEP)]
        s = jnp.concatenate(
            [
                jnp.concatenate([f_ref[3 * part + k, row, :].astype(BF16) for row in rows for k in range(3)], axis=1)
                for part in range(2)
            ],
            axis=0,
        )
        hid = jnp.maximum(dot(w1, s) + b1, 0.0).astype(BF16)
        out = dot(w2, hid)
        out = out - jnp.clip(out, -0.01, 0.01)
        for n, row in enumerate(rows):
            for part in range(2):
                for k in range(3):
                    lane = 384 * n + 128 * k
                    h_ref[3 * part + k, row, :] = out[96 * part : 96 * part + 96, lane : lane + 128]
        return 0

    lax.fori_loop(0, 24 // MIX_STEP, mix, 0, unroll=3)

    def inverse(g, _):
        l = pl.ds(pl.multiple_of(g * 768, 768), 768)
        hb = jnp.concatenate([h_ref[k, l, :].astype(BF16) for k in range(6)], axis=1)
        out = dot(ti_ref[...], hb, ((1,), (1,)))
        o_ref[:, :, l] = out.astype(BF16).reshape(16, 48, 768)
        return 0

    lax.fori_loop(0, GROUPS // 2, inverse, 0, unroll=3)


def spectral(layer, r, wa, ba, wb, tf, ti):
    def kernel(*refs):
        spectral_kernel(layer, *refs)

    return pl.pallas_call(
        kernel,
        out_shape=jax.ShapeDtypeStruct(r.shape, BF16),
        in_specs=[VM] * 6,
        out_specs=VM,
        scratch_shapes=[
            pltpu.VMEM((384, 768), BF16),
            pltpu.VMEM((6, 2304, 128), F32),
            pltpu.VMEM((6, 2304, 128), F32),
        ],
        compiler_params=params(SPECTRAL_MIB),
        cost_estimate=cost(12 * 10**9, 10**7),
        name="spectral",
    )(r, wa, ba, wb, tf, ti)


def spatial_kernel(first, last, *refs):
    refs = list(refs)
    scale = 1.0 if first else layer_scale(refs.pop(0))
    y_ref, v_ref, n_ref, tl_ref, u_ref, st_ref, z_ref, sum_ref, sq_ref = refs
    sum_ref[...] = jnp.zeros_like(sum_ref)
    sq_ref[...] = jnp.zeros_like(sq_ref)

    def inverse(g, _):
        l = lanes_of(g)
        gather_rows(y_ref, l, z_ref)
        sp = natural_rows(dot(z_ref[...], tl_ref[...])).reshape(16, 24, 768)
        d = chans_of(g)
        u = sp + n_ref[d].astype(F32) + v_ref[d].astype(F32) * scale
        u_ref[d] = u.astype(BF16)
        sum_ref[...] += jnp.sum(u, axis=0)
        sq_ref[...] += jnp.sum(u * u, axis=0)
        return 0

    lax.fori_loop(0, GROUPS, inverse, 0, unroll=6)
    if last:
        st_ref[...] = jnp.broadcast_to(band_energy(sq_ref[...]).reshape(1, 1, 1), st_ref.shape)
    else:
        put_stats(st_ref, sum_ref[...], sq_ref[...])


def spatial(first, last, extra, y, v, n, tl):
    plane = v.shape[1:]
    stats = jax.ShapeDtypeStruct((128, 1, 128), F32) if last else jax.ShapeDtypeStruct((2, *plane), BF16)

    def kernel(*refs):
        spatial_kernel(first, last, *refs)

    return pl.pallas_call(
        kernel,
        out_shape=(jax.ShapeDtypeStruct(v.shape, BF16), stats),
        in_specs=[VM] * (len(extra) + 4),
        out_specs=(VM, VM),
        scratch_shapes=[pltpu.VMEM((384, 768), BF16), pltpu.VMEM(plane, F32), pltpu.VMEM(plane, F32)],
        compiler_params=params(SPATIAL_MIB),
        cost_estimate=cost(3 * 10**9, 15 * 10**6),
        name="spatial",
    )(*extra, y, v, n, tl)


def final_kernel(pay_ref, energy_ref, u_ref, o_hbm, o_ref, sems):
    def store(g):
        return pltpu.make_async_copy(o_ref.at[chans_of(g)], o_hbm.at[chans_of(g)], sems.at[g])

    target = jnp.sum(pay_ref[...], axis=0)[0:1]
    energy = jnp.sum(energy_ref[...], axis=0)
    scale = jnp.sqrt(target / energy)[0, 0]

    def group(g, _):
        o_ref[chans_of(g)] = (u_ref[chans_of(g)].astype(F32) * scale).astype(BF16)
        store(g).start()
        return 0

    lax.fori_loop(0, GROUPS, group, 0)

    def drain(g, _):
        store(g).wait()
        return 0

    lax.fori_loop(0, GROUPS, drain, 0)


def final_scale(pay, energy, u):
    return pl.pallas_call(
        final_kernel,
        out_shape=jax.ShapeDtypeStruct(u.shape, BF16),
        in_specs=[VM] * 3,
        out_specs=pl.BlockSpec(memory_space=pl.ANY),
        scratch_shapes=[pltpu.VMEM(u.shape, BF16), pltpu.SemaphoreType.DMA((GROUPS,))],
        compiler_params=params(12),
        cost_estimate=cost(10**7, 7 * 10**6),
        name="final_scale",
    )(pay, energy, u)


def swap(x, axes):
    return lax.all_to_all(x, axes, split_axis=0, concat_axis=0, tiled=True)


def ring(x, axis, step):
    n = lax.axis_size(axis)
    return lax.ppermute(x, axis, [(i, (i + step) % n) for i in range(n)])


def stat_parts(stats):
    pair = (stats.astype(F32) + ring(stats, CH[1], 1).astype(F32)).astype(BF16)
    return [pair] + [ring(pair, CH[0], step) for step in range(1, lax.axis_size(CH[0]))]


def per_device(field_in, ln_gain, ln_shift, mix_first, mix_bias, mix_second):
    tf, ti, tw, tl = (jnp.asarray(t) for t in host_tables())
    layers = mix_first.shape[0]
    bias = mix_bias.reshape(layers, 2, -1)
    current, stats = field_in, first_stats(field_in)
    band, scales = None, []
    for layer in range(layers):
        parts = stat_parts(stats)
        if layer == 0:
            normed, lon, band = norm_lon(layer, ln_gain, ln_shift, current, tw, *parts)
        else:
            sums, pay = band_sums(band, parts)
            scales = [swap(pay, LAT)]
            normed, lon = norm_lon(layer, ln_gain, ln_shift, current, tw, *scales, sums)
        back = spectral(layer, swap(lon, LAT), mix_first, bias, mix_second, tf, ti)
        first, last = layer == 0, layer == layers - 1
        current, stats = spatial(first, last, scales, swap(back, LAT), current, normed, tl)
    return final_scale(scales[0], swap(stats, LAT_CH), current)


def solution(mesh):
    finer = Mesh(mesh.devices.reshape(4, 4, 4, 2), LAT_CH)
    in_specs = (
        P(CH, LAT, None),
        P(None, CH),
        P(None, CH),
        P(None, None, CH, None, None),
        P(None, None, CH, None),
        P(None, None, CH, None, None),
    )
    return jax.shard_map(
        per_device, mesh=finer, in_specs=in_specs, out_specs=P(CH, LAT, None), check_vma=False
    )
```

```python
import math

import jax
import jax.numpy as jnp
import numpy as np
from jax import lax
from jax.experimental import pallas as pl
from jax.experimental.pallas import tpu as pltpu
from jax.sharding import Mesh
from jax.sharding import PartitionSpec as P

CH = ("ch_0", "ch_1")
LAT = ("lat_0", "lat_1")
LAT_CH = LAT + CH
NORM_EPS = 1e-05
CH_ALL = 768
GROUPS = 6
MIX_STEP = 8
NORM_UNROLL = 1
NORM_MIB, SPECTRAL_MIB, SPATIAL_MIB = 12, 24, 12
F32, BF16 = jnp.float32, jnp.bfloat16
VM = pl.BlockSpec(memory_space=pltpu.VMEM)
SM = pl.BlockSpec(memory_space=pltpu.SMEM)


PIECE_ROWS = np.r_[0:16, 24:40, 16:24, 40:48]


def host_tables():
    def trig(length, freqs):
        n = np.arange(length)
        a = (n[:, None] * freqs[None, :] % length) * (2.0 * math.pi / length)
        s = 1.0 / math.sqrt(length)
        return (np.cos(a) * s).astype(jnp.bfloat16), (np.sin(a) * s).astype(jnp.bfloat16)

    def pieces(table):
        return table.reshape(2, 16, 24, 768).transpose(1, 0, 2, 3).reshape(16, 48, 768)[:, PIECE_ROWS].reshape(768, 768)

    c, s = trig(384, np.arange(384))
    lat = np.block([[c, -s], [s, c]])
    c, s = trig(768, np.arange(384))
    lon = np.concatenate([c.T, -s.T], 0)
    twice = np.where(np.arange(768) % 384 == 0, 1.0, 2.0)[:, None]
    weighted = (lon.astype(np.float32) * twice).astype(jnp.bfloat16)
    return lat, pieces(lat), pieces(lon), weighted


def lanes_of(g):
    return pl.ds(pl.multiple_of(g * 384, 384), 384)


def chans_of(g):
    return pl.ds(pl.multiple_of(g * 16, 16), 16)


def exchange(xs, unit):
    n, tile = len(xs), 128
    tiles = n * unit // tile
    lane = lax.broadcasted_iota(jnp.int32, (16, tile), 1).astype(F32).astype(BF16)
    cuts = {k: lane >= jnp.asarray(k, BF16) for k in range(8, tile, 8)}

    def by_block(t, pick):
        out = pick(t * tile // unit)
        for block in range(t * tile // unit + 1, -(-(t + 1) * tile // unit)):
            out = jnp.where(cuts[block * unit - t * tile], pick(block), out)
        return out

    moved = []
    for s in range(n):
        held = [by_block(t, lambda b, t=t: xs[(b + s) % n][:, tile * t : tile * t + tile]) for t in range(tiles)]
        whole, part = divmod(s * unit, tile)
        if part:
            turned = [pltpu.roll(h, part, 1) for h in held]
            moved.append(
                [jnp.where(cuts[part], turned[(t - whole) % tiles], turned[(t - whole - 1) % tiles]) for t in range(tiles)]
            )
        else:
            moved.append([held[(t - whole) % tiles] for t in range(tiles)])
    return [
        jnp.concatenate([by_block(t, lambda b, t=t: moved[(b - c) % n][t]) for t in range(tiles)], axis=1)
        for c in range(n)
    ]


def gather_rows(x_ref, lanes, g_ref):
    for part in range(2):
        cols = slice(384 * part, 384 * part + 384)
        for c, v in enumerate(exchange([x_ref[p, 16 * part : 16 * part + 16, lanes] for p in range(16)], 24)):
            row = 48 * (c // 2) + 16 * (c % 2)
            g_ref[row : row + 16, cols] = v
    tails = exchange([x_ref[p, 32:48, lanes] for p in range(16)], 24)
    for c in range(0, 16, 2):
        row = 24 * c + 32
        for part in range(2):
            half = slice(8 * part, 8 * part + 8)
            g_ref[row : row + 16, 384 * part : 384 * part + 384] = jnp.concatenate(
                [tails[c][half], tails[c + 1][half]], axis=0
            )


def natural_rows(x):
    x = x.reshape(8, 6, 8, 768)
    return jnp.concatenate([x[:, :2], x[:, 4:5], x[:, 2:4], x[:, 5:]], axis=1).reshape(384, 768)


def dot(a, b, dims=((1,), (0,))):
    return lax.dot_general(a, b, (dims, ((), ())), preferred_element_type=F32)


def params(mib):
    return pltpu.CompilerParams(vmem_limit_bytes=mib << 20)


def cost(flops, moved):
    return pl.CostEstimate(flops=flops, bytes_accessed=moved, transcendentals=0)


def put_stats(st_ref, sums, squares):
    st_ref[0] = sums
    st_ref[1] = squares


def band_energy(squares):
    rows = squares.shape[0]
    first_row = lax.axis_index(LAT) * rows
    row_pos = (first_row + lax.broadcasted_iota(jnp.int32, squares.shape, 0)).astype(F32)
    area = jnp.cos((row_pos + 0.5) * (math.pi / (rows * lax.axis_size(LAT))) - 0.5 * math.pi)
    return jnp.sum(area * squares, keepdims=True)


def first_stats_kernel(v_ref, st_ref, sum_ref, sq_ref):
    sum_ref[...] = jnp.zeros_like(sum_ref)
    sq_ref[...] = jnp.zeros_like(sq_ref)

    def group(g, _):
        v = v_ref[chans_of(g)].astype(F32)
        sum_ref[...] += jnp.sum(v, axis=0)
        sq_ref[...] += jnp.sum(v * v, axis=0)
        return 0

    lax.fori_loop(0, GROUPS, group, 0)
    put_stats(st_ref, sum_ref[...], sq_ref[...])


def first_stats(v):
    plane = v.shape[1:]
    return pl.pallas_call(
        first_stats_kernel,
        out_shape=jax.ShapeDtypeStruct((2, *plane), F32),
        in_specs=[VM],
        out_specs=VM,
        scratch_shapes=[pltpu.VMEM(plane, F32), pltpu.VMEM(plane, F32)],
        compiler_params=params(8),
        cost_estimate=cost(5 * 10**9, 10**7),
        name="first_stats",
    )(v)


def gather_stats(st_refs):
    return tuple(sum(st_ref[i].astype(F32) for st_ref in st_refs) for i in range(2))


def band_kernel(first_ref, *refs):
    *st_refs, sums_ref, pay_ref = refs
    total, squares = gather_stats(st_refs)
    sums_ref[0] = total
    sums_ref[1] = squares
    both = jnp.concatenate([first_ref[...], jnp.broadcast_to(band_energy(squares), (1, 128))], axis=0)
    pay_ref[...] = jnp.broadcast_to(both[None], pay_ref.shape)


def band_sums(first, parts):
    return pl.pallas_call(
        band_kernel,
        out_shape=(jax.ShapeDtypeStruct(parts[0].shape, F32), jax.ShapeDtypeStruct((16, 2, 128), F32)),
        in_specs=[VM] * (1 + len(parts)),
        out_specs=(VM, VM),
        compiler_params=params(8),
        cost_estimate=cost(10**6, 10**6),
        name="band_sums",
    )(first, *parts)


def layer_scale(pay_ref):
    both = jnp.sum(pay_ref[...], axis=0)
    return jnp.sqrt(both[0:1] / both[1:2])[0, 0]


def norm_kernel(layer, gain_ref, shift_ref, v_ref, tw_ref, *refs):
    if layer == 0:
        *st_refs, n_ref, o_ref, band_ref, mean_ref, inv_ref = refs
        scale = 1.0
        total, squares = gather_stats(st_refs)
        band_ref[...] = jnp.broadcast_to(band_energy(squares), (1, 128))
    else:
        pay_ref, sums_ref, n_ref, o_ref, mean_ref, inv_ref = refs
        scale = layer_scale(pay_ref)
        total, squares = sums_ref[0], sums_ref[1]
    mean = total / CH_ALL
    spread = squares / CH_ALL - mean * mean
    mean_ref[...] = mean
    inv_ref[...] = scale * lax.rsqrt(spread * (scale * scale) + NORM_EPS)

    def group(g, _):
        mean, inv = mean_ref[...], inv_ref[...]
        rows = []
        for i in range(32):
            c = g * 32 + i
            rows.append((v_ref[c].astype(F32) - mean) * inv * gain_ref[layer, c] + shift_ref[layer, c])
        x = jnp.concatenate(rows, axis=0).astype(BF16)
        n_ref[pl.ds(pl.multiple_of(g * 32, 32), 32)] = x.astype(F32).reshape(32, 24, 768).astype(BF16)
        out = dot(tw_ref[...], x, ((1,), (1,)))
        o_ref[:, :, pl.ds(pl.multiple_of(g * 768, 768), 768)] = out.astype(BF16).reshape(16, 48, 768)
        return 0

    lax.fori_loop(0, GROUPS // 2, group, 0, unroll=NORM_UNROLL)


def norm_lon(layer, gain, shift, v, tw, *stats):
    plane = v.shape[1:]
    outs = [jax.ShapeDtypeStruct(v.shape, BF16), jax.ShapeDtypeStruct((16, 48, 2304), BF16)]

    if layer == 0:
        outs.append(jax.ShapeDtypeStruct((1, 128), F32))

    def kernel(*refs):
        norm_kernel(layer, *refs)

    return pl.pallas_call(
        kernel,
        out_shape=tuple(outs),
        in_specs=[SM, SM] + [VM] * (2 + len(stats)),
        out_specs=(VM,) * len(outs),
        scratch_shapes=[pltpu.VMEM(plane, F32), pltpu.VMEM(plane, F32)],
        compiler_params=params(NORM_MIB),
        cost_estimate=cost(3 * 10**9, 10**7),
        name="norm_lon",
    )(gain, shift, v, tw, *stats)


def complex_weight(w_ref, layer):
    re, im = (w_ref[layer, part, 0].astype(F32).T for part in range(2))
    rows = [jnp.concatenate([re, -im], axis=1), jnp.concatenate([im, re], axis=1)]
    return jnp.concatenate(rows, axis=0).astype(BF16)


def spectral_kernel(layer, r_ref, wa_ref, ba_ref, wb_ref, tf_ref, ti_ref, o_ref, g_ref, f_ref, h_ref):
    def forward(g, _):
        l = lanes_of(g)
        gather_rows(r_ref, l, g_ref)
        prod = natural_rows(dot(g_ref[...], tf_ref[...]))
        for k in range(6):
            f_ref[k, l, :] = prod[:, 128 * k : 128 * k + 128]
        return 0

    lax.fori_loop(0, GROUPS, forward, 0, unroll=6)
    w1, w2 = complex_weight(wa_ref, layer), complex_weight(wb_ref, layer)
    b1 = jnp.concatenate([ba_ref[layer, part : part + 1].astype(F32).T for part in range(2)], axis=0)

    def mix(i, _):
        rows = [pl.ds(i * MIX_STEP + k, 96, stride=24) for k in range(MIX_STEP)]
        s = jnp.concatenate(
            [
                jnp.concatenate([f_ref[3 * part + k, row, :].astype(BF16) for row in rows for k in range(3)], axis=1)
                for part in range(2)
            ],
            axis=0,
        )
        hid = jnp.maximum(dot(w1, s) + b1, 0.0).astype(BF16)
        out = dot(w2, hid)
        out = out - jnp.clip(out, -0.01, 0.01)
        for n, row in enumerate(rows):
            for part in range(2):
                for k in range(3):
                    lane = 384 * n + 128 * k
                    h_ref[3 * part + k, row, :] = out[96 * part : 96 * part + 96, lane : lane + 128]
        return 0

    lax.fori_loop(0, 24 // MIX_STEP, mix, 0, unroll=3)

    def inverse(g, _):
        l = pl.ds(pl.multiple_of(g * 768, 768), 768)
        hb = jnp.concatenate([h_ref[k, l, :].astype(BF16) for k in range(6)], axis=1)
        out = dot(ti_ref[...], hb, ((1,), (1,)))
        o_ref[:, :, l] = out.astype(BF16).reshape(16, 48, 768)
        return 0

    lax.fori_loop(0, GROUPS // 2, inverse, 0, unroll=3)


def spectral(layer, r, wa, ba, wb, tf, ti):
    def kernel(*refs):
        spectral_kernel(layer, *refs)

    return pl.pallas_call(
        kernel,
        out_shape=jax.ShapeDtypeStruct(r.shape, BF16),
        in_specs=[VM] * 6,
        out_specs=VM,
        scratch_shapes=[
            pltpu.VMEM((384, 768), BF16),
            pltpu.VMEM((6, 2304, 128), F32),
            pltpu.VMEM((6, 2304, 128), F32),
        ],
        compiler_params=params(SPECTRAL_MIB),
        cost_estimate=cost(12 * 10**9, 10**7),
        name="spectral",
    )(r, wa, ba, wb, tf, ti)


def spatial_kernel(first, last, *refs):
    refs = list(refs)
    scale = 1.0 if first else layer_scale(refs.pop(0))
    y_ref, v_ref, n_ref, tl_ref, u_ref, st_ref, z_ref, sum_ref, sq_ref = refs
    sum_ref[...] = jnp.zeros_like(sum_ref)
    sq_ref[...] = jnp.zeros_like(sq_ref)

    def inverse(g, _):
        l = lanes_of(g)
        gather_rows(y_ref, l, z_ref)
        sp = natural_rows(dot(z_ref[...], tl_ref[...])).reshape(16, 24, 768)
        d = chans_of(g)
        u = sp + n_ref[d].astype(F32) + v_ref[d].astype(F32) * scale
        u_ref[d] = u.astype(BF16)
        sum_ref[...] += jnp.sum(u, axis=0)
        sq_ref[...] += jnp.sum(u * u, axis=0)
        return 0

    lax.fori_loop(0, GROUPS, inverse, 0, unroll=6)
    if last:
        st_ref[...] = jnp.broadcast_to(band_energy(sq_ref[...]).reshape(1, 1, 1), st_ref.shape)
    else:
        put_stats(st_ref, sum_ref[...], sq_ref[...])


def spatial(first, last, extra, y, v, n, tl):
    plane = v.shape[1:]
    stats = jax.ShapeDtypeStruct((128, 1, 128), F32) if last else jax.ShapeDtypeStruct((2, *plane), F32)

    def kernel(*refs):
        spatial_kernel(first, last, *refs)

    return pl.pallas_call(
        kernel,
        out_shape=(jax.ShapeDtypeStruct(v.shape, BF16), stats),
        in_specs=[VM] * (len(extra) + 4),
        out_specs=(VM, VM),
        scratch_shapes=[pltpu.VMEM((384, 768), BF16), pltpu.VMEM(plane, F32), pltpu.VMEM(plane, F32)],
        compiler_params=params(SPATIAL_MIB),
        cost_estimate=cost(3 * 10**9, 15 * 10**6),
        name="spatial",
    )(*extra, y, v, n, tl)


def final_kernel(pay_ref, energy_ref, u_ref, o_hbm, o_ref, sems):
    def store(g):
        return pltpu.make_async_copy(o_ref.at[chans_of(g)], o_hbm.at[chans_of(g)], sems.at[g])

    target = jnp.sum(pay_ref[...], axis=0)[0:1]
    energy = jnp.sum(energy_ref[...], axis=0)
    scale = jnp.sqrt(target / energy)[0, 0]

    def group(g, _):
        o_ref[chans_of(g)] = (u_ref[chans_of(g)].astype(F32) * scale).astype(BF16)
        store(g).start()
        return 0

    lax.fori_loop(0, GROUPS, group, 0)

    def drain(g, _):
        store(g).wait()
        return 0

    lax.fori_loop(0, GROUPS, drain, 0)


def final_scale(pay, energy, u):
    return pl.pallas_call(
        final_kernel,
        out_shape=jax.ShapeDtypeStruct(u.shape, BF16),
        in_specs=[VM] * 3,
        out_specs=pl.BlockSpec(memory_space=pl.ANY),
        scratch_shapes=[pltpu.VMEM(u.shape, BF16), pltpu.SemaphoreType.DMA((GROUPS,))],
        compiler_params=params(12),
        cost_estimate=cost(10**7, 7 * 10**6),
        name="final_scale",
    )(pay, energy, u)


def swap(x, axes):
    return lax.all_to_all(x, axes, split_axis=0, concat_axis=0, tiled=True)


def ring(x, axis, step):
    n = lax.axis_size(axis)
    return lax.ppermute(x, axis, [(i, (i + step) % n) for i in range(n)])


def stat_parts(stats):
    pair = (stats + ring(stats, CH[1], 1)).astype(BF16)
    return [pair] + [ring(pair, CH[0], step) for step in range(1, lax.axis_size(CH[0]))]


def per_device(field_in, ln_gain, ln_shift, mix_first, mix_bias, mix_second):
    tf, ti, tw, tl = (jnp.asarray(t) for t in host_tables())
    layers = mix_first.shape[0]
    bias = mix_bias.reshape(layers, 2, -1)
    current, stats = field_in, first_stats(field_in)
    band, scales = None, []
    for layer in range(layers):
        parts = stat_parts(stats)
        if layer == 0:
            normed, lon, band = norm_lon(layer, ln_gain, ln_shift, current, tw, *parts)
        else:
            sums, pay = band_sums(band, parts)
            scales = [swap(pay, LAT)]
            normed, lon = norm_lon(layer, ln_gain, ln_shift, current, tw, *scales, sums)
        back = spectral(layer, swap(lon, LAT), mix_first, bias, mix_second, tf, ti)
        first, last = layer == 0, layer == layers - 1
        current, stats = spatial(first, last, scales, swap(back, LAT), current, normed, tl)
    return final_scale(scales[0], swap(stats, LAT_CH), current)


def solution(mesh):
    finer = Mesh(mesh.devices.reshape(4, 4, 4, 2), LAT_CH)
    in_specs = (
        P(CH, LAT, None),
        P(None, CH),
        P(None, CH),
        P(None, None, CH, None, None),
        P(None, None, CH, None),
        P(None, None, CH, None, None),
    )
    return jax.shard_map(
        per_device, mesh=finer, in_specs=in_specs, out_specs=P(CH, LAT, None), check_vma=False
    )
```

```python
import math

import jax
import jax.numpy as jnp
import numpy as np
from jax import lax
from jax.experimental import pallas as pl
from jax.experimental.pallas import tpu as pltpu
from jax.sharding import Mesh
from jax.sharding import PartitionSpec as P

CH = ("ch_0", "ch_1")
LAT = ("lat_0", "lat_1")
LAT_CH = LAT + CH
NORM_EPS = 1e-05
CH_ALL = 768
GROUPS = 6
MIX_STEP = 4
NORM_UNROLL = 3
NORM_MIB, SPECTRAL_MIB, SPATIAL_MIB = 12, 24, 12
F32, BF16 = jnp.float32, jnp.bfloat16
VM = pl.BlockSpec(memory_space=pltpu.VMEM)
SM = pl.BlockSpec(memory_space=pltpu.SMEM)


PIECE_ROWS = np.r_[0:16, 24:40, 16:24, 40:48]


def host_tables():
    def trig(length, freqs):
        n = np.arange(length)
        a = (n[:, None] * freqs[None, :] % length) * (2.0 * math.pi / length)
        s = 1.0 / math.sqrt(length)
        return (np.cos(a) * s).astype(jnp.bfloat16), (np.sin(a) * s).astype(jnp.bfloat16)

    def pieces(table):
        return table.reshape(2, 16, 24, 768).transpose(1, 0, 2, 3).reshape(16, 48, 768)[:, PIECE_ROWS].reshape(768, 768)

    c, s = trig(384, np.arange(384))
    lat = np.block([[c, -s], [s, c]])
    c, s = trig(768, np.arange(384))
    lon = np.concatenate([c.T, -s.T], 0)
    twice = np.where(np.arange(768) % 384 == 0, 1.0, 2.0)[:, None]
    weighted = (lon.astype(np.float32) * twice).astype(jnp.bfloat16)
    return lat, pieces(lat), pieces(lon), weighted


def lanes_of(g):
    return pl.ds(pl.multiple_of(g * 384, 384), 384)


def chans_of(g):
    return pl.ds(pl.multiple_of(g * 16, 16), 16)


def exchange(xs, unit):
    n, tile = len(xs), 128
    tiles = n * unit // tile
    lane = lax.broadcasted_iota(jnp.int32, (16, tile), 1).astype(F32).astype(BF16)
    cuts = {k: lane >= jnp.asarray(k, BF16) for k in range(8, tile, 8)}

    def by_block(t, pick):
        out = pick(t * tile // unit)
        for block in range(t * tile // unit + 1, -(-(t + 1) * tile // unit)):
            out = jnp.where(cuts[block * unit - t * tile], pick(block), out)
        return out

    moved = []
    for s in range(n):
        held = [by_block(t, lambda b, t=t: xs[(b + s) % n][:, tile * t : tile * t + tile]) for t in range(tiles)]
        whole, part = divmod(s * unit, tile)
        if part:
            turned = [pltpu.roll(h, part, 1) for h in held]
            moved.append(
                [jnp.where(cuts[part], turned[(t - whole) % tiles], turned[(t - whole - 1) % tiles]) for t in range(tiles)]
            )
        else:
            moved.append([held[(t - whole) % tiles] for t in range(tiles)])
    return [
        jnp.concatenate([by_block(t, lambda b, t=t: moved[(b - c) % n][t]) for t in range(tiles)], axis=1)
        for c in range(n)
    ]


def gather_rows(x_ref, lanes, g_ref):
    for part in range(2):
        cols = slice(384 * part, 384 * part + 384)
        for c, v in enumerate(exchange([x_ref[p, 16 * part : 16 * part + 16, lanes] for p in range(16)], 24)):
            row = 48 * (c // 2) + 16 * (c % 2)
            g_ref[row : row + 16, cols] = v
    tails = exchange([x_ref[p, 32:48, lanes] for p in range(16)], 24)
    for c in range(0, 16, 2):
        row = 24 * c + 32
        for part in range(2):
            half = slice(8 * part, 8 * part + 8)
            g_ref[row : row + 16, 384 * part : 384 * part + 384] = jnp.concatenate(
                [tails[c][half], tails[c + 1][half]], axis=0
            )


def natural_rows(x):
    x = x.reshape(8, 6, 8, 768)
    return jnp.concatenate([x[:, :2], x[:, 4:5], x[:, 2:4], x[:, 5:]], axis=1).reshape(384, 768)


def dot(a, b, dims=((1,), (0,))):
    return lax.dot_general(a, b, (dims, ((), ())), preferred_element_type=F32)


def params(mib):
    return pltpu.CompilerParams(vmem_limit_bytes=mib << 20)


def cost(flops, moved):
    return pl.CostEstimate(flops=flops, bytes_accessed=moved, transcendentals=0)


def put_stats(st_ref, sums, squares):
    st_ref[0] = sums.astype(BF16)
    st_ref[1] = squares.astype(BF16)


def band_energy(squares):
    rows = squares.shape[0]
    first_row = lax.axis_index(LAT) * rows
    row_pos = (first_row + lax.broadcasted_iota(jnp.int32, squares.shape, 0)).astype(F32)
    area = jnp.cos((row_pos + 0.5) * (math.pi / (rows * lax.axis_size(LAT))) - 0.5 * math.pi)
    return jnp.sum(area * squares, keepdims=True)


def first_stats_kernel(v_ref, st_ref, sum_ref, sq_ref):
    sum_ref[...] = jnp.zeros_like(sum_ref)
    sq_ref[...] = jnp.zeros_like(sq_ref)

    def group(g, _):
        v = v_ref[chans_of(g)].astype(F32)
        sum_ref[...] += jnp.sum(v, axis=0)
        sq_ref[...] += jnp.sum(v * v, axis=0)
        return 0

    lax.fori_loop(0, GROUPS, group, 0)
    put_stats(st_ref, sum_ref[...], sq_ref[...])


def first_stats(v):
    plane = v.shape[1:]
    return pl.pallas_call(
        first_stats_kernel,
        out_shape=jax.ShapeDtypeStruct((2, *plane), BF16),
        in_specs=[VM],
        out_specs=VM,
        scratch_shapes=[pltpu.VMEM(plane, F32), pltpu.VMEM(plane, F32)],
        compiler_params=params(8),
        cost_estimate=cost(5 * 10**9, 10**7),
        name="first_stats",
    )(v)


def gather_stats(st_refs):
    return tuple(sum(st_ref[i].astype(F32) for st_ref in st_refs) for i in range(2))


def band_kernel(first_ref, *refs):
    *st_refs, sums_ref, pay_ref = refs
    total, squares = gather_stats(st_refs)
    sums_ref[0] = total
    sums_ref[1] = squares
    both = jnp.concatenate([first_ref[...], jnp.broadcast_to(band_energy(squares), (1, 128))], axis=0)
    pay_ref[...] = jnp.broadcast_to(both[None], pay_ref.shape)


def band_sums(first, parts):
    return pl.pallas_call(
        band_kernel,
        out_shape=(jax.ShapeDtypeStruct(parts[0].shape, F32), jax.ShapeDtypeStruct((16, 2, 128), F32)),
        in_specs=[VM] * (1 + len(parts)),
        out_specs=(VM, VM),
        compiler_params=params(8),
        cost_estimate=cost(10**6, 10**6),
        name="band_sums",
    )(first, *parts)


def layer_scale(pay_ref):
    both = jnp.sum(pay_ref[...], axis=0)
    return jnp.sqrt(both[0:1] / both[1:2])[0, 0]


def norm_kernel(layer, gain_ref, shift_ref, v_ref, tw_ref, *refs):
    if layer == 0:
        *st_refs, n_ref, o_ref, band_ref, mean_ref, inv_ref = refs
        scale = 1.0
        total, squares = gather_stats(st_refs)
        band_ref[...] = jnp.broadcast_to(band_energy(squares), (1, 128))
    else:
        pay_ref, sums_ref, n_ref, o_ref, mean_ref, inv_ref = refs
        scale = layer_scale(pay_ref)
        total, squares = sums_ref[0], sums_ref[1]
    mean = total / CH_ALL
    spread = squares / CH_ALL - mean * mean
    mean_ref[...] = mean
    inv_ref[...] = scale * lax.rsqrt(spread * (scale * scale) + NORM_EPS)

    def group(g, _):
        mean, inv = mean_ref[...], inv_ref[...]
        rows = []
        for i in range(32):
            c = g * 32 + i
            rows.append((v_ref[c].astype(F32) - mean) * inv * gain_ref[layer, c] + shift_ref[layer, c])
        x = jnp.concatenate(rows, axis=0).astype(BF16)
        n_ref[pl.ds(pl.multiple_of(g * 32, 32), 32)] = x.astype(F32).reshape(32, 24, 768).astype(BF16)
        out = dot(tw_ref[...], x, ((1,), (1,)))
        o_ref[:, :, pl.ds(pl.multiple_of(g * 768, 768), 768)] = out.astype(BF16).reshape(16, 48, 768)
        return 0

    lax.fori_loop(0, GROUPS // 2, group, 0, unroll=NORM_UNROLL)


def norm_lon(layer, gain, shift, v, tw, *stats):
    plane = v.shape[1:]
    outs = [jax.ShapeDtypeStruct(v.shape, BF16), jax.ShapeDtypeStruct((16, 48, 2304), BF16)]

    if layer == 0:
        outs.append(jax.ShapeDtypeStruct((1, 128), F32))

    def kernel(*refs):
        norm_kernel(layer, *refs)

    return pl.pallas_call(
        kernel,
        out_shape=tuple(outs),
        in_specs=[SM, SM] + [VM] * (2 + len(stats)),
        out_specs=(VM,) * len(outs),
        scratch_shapes=[pltpu.VMEM(plane, F32), pltpu.VMEM(plane, F32)],
        compiler_params=params(NORM_MIB),
        cost_estimate=cost(3 * 10**9, 10**7),
        name="norm_lon",
    )(gain, shift, v, tw, *stats)


def complex_weight(w_ref, layer):
    re, im = (w_ref[layer, part, 0].astype(F32).T for part in range(2))
    rows = [jnp.concatenate([re, -im], axis=1), jnp.concatenate([im, re], axis=1)]
    return jnp.concatenate(rows, axis=0).astype(BF16)


def spectral_kernel(layer, r_ref, wa_ref, ba_ref, wb_ref, tf_ref, ti_ref, o_ref, g_ref, f_ref, h_ref):
    def forward(g, _):
        l = lanes_of(g)
        gather_rows(r_ref, l, g_ref)
        prod = natural_rows(dot(g_ref[...], tf_ref[...]))
        for k in range(6):
            f_ref[k, l, :] = prod[:, 128 * k : 128 * k + 128]
        return 0

    lax.fori_loop(0, GROUPS, forward, 0, unroll=6)
    w1, w2 = complex_weight(wa_ref, layer), complex_weight(wb_ref, layer)
    b1 = jnp.concatenate([ba_ref[layer, part : part + 1].astype(F32).T for part in range(2)], axis=0)

    def mix(i, _):
        rows = [pl.ds(i * MIX_STEP + k, 96, stride=24) for k in range(MIX_STEP)]
        s = jnp.concatenate(
            [
                jnp.concatenate([f_ref[3 * part + k, row, :].astype(BF16) for row in rows for k in range(3)], axis=1)
                for part in range(2)
            ],
            axis=0,
        )
        hid = jnp.maximum(dot(w1, s) + b1, 0.0).astype(BF16)
        out = dot(w2, hid)
        out = out - jnp.clip(out, -0.01, 0.01)
        for n, row in enumerate(rows):
            for part in range(2):
                for k in range(3):
                    lane = 384 * n + 128 * k
                    h_ref[3 * part + k, row, :] = out[96 * part : 96 * part + 96, lane : lane + 128]
        return 0

    lax.fori_loop(0, 24 // MIX_STEP, mix, 0, unroll=6)

    def inverse(g, _):
        l = pl.ds(pl.multiple_of(g * 768, 768), 768)
        hb = jnp.concatenate([h_ref[k, l, :].astype(BF16) for k in range(6)], axis=1)
        out = dot(ti_ref[...], hb, ((1,), (1,)))
        o_ref[:, :, l] = out.astype(BF16).reshape(16, 48, 768)
        return 0

    lax.fori_loop(0, GROUPS // 2, inverse, 0, unroll=3)


def spectral(layer, r, wa, ba, wb, tf, ti):
    def kernel(*refs):
        spectral_kernel(layer, *refs)

    return pl.pallas_call(
        kernel,
        out_shape=jax.ShapeDtypeStruct(r.shape, BF16),
        in_specs=[VM] * 6,
        out_specs=VM,
        scratch_shapes=[
            pltpu.VMEM((384, 768), BF16),
            pltpu.VMEM((6, 2304, 128), F32),
            pltpu.VMEM((6, 2304, 128), F32),
        ],
        compiler_params=params(SPECTRAL_MIB),
        cost_estimate=cost(12 * 10**9, 10**7),
        name="spectral",
    )(r, wa, ba, wb, tf, ti)


def spatial_kernel(first, last, *refs):
    refs = list(refs)
    scale = 1.0 if first else layer_scale(refs.pop(0))
    y_ref, v_ref, n_ref, tl_ref, u_ref, st_ref, z_ref, sum_ref, sq_ref = refs
    sum_ref[...] = jnp.zeros_like(sum_ref)
    sq_ref[...] = jnp.zeros_like(sq_ref)

    def inverse(g, _):
        l = lanes_of(g)
        gather_rows(y_ref, l, z_ref)
        sp = natural_rows(dot(z_ref[...], tl_ref[...])).reshape(16, 24, 768)
        d = chans_of(g)
        u = sp + n_ref[d].astype(F32) + v_ref[d].astype(F32) * scale
        u_ref[d] = u.astype(BF16)
        sum_ref[...] += jnp.sum(u, axis=0)
        sq_ref[...] += jnp.sum(u * u, axis=0)
        return 0

    lax.fori_loop(0, GROUPS, inverse, 0, unroll=6)
    if last:
        st_ref[...] = jnp.broadcast_to(band_energy(sq_ref[...]).reshape(1, 1, 1), st_ref.shape)
    else:
        put_stats(st_ref, sum_ref[...], sq_ref[...])


def spatial(first, last, extra, y, v, n, tl):
    plane = v.shape[1:]
    stats = jax.ShapeDtypeStruct((128, 1, 128), F32) if last else jax.ShapeDtypeStruct((2, *plane), BF16)

    def kernel(*refs):
        spatial_kernel(first, last, *refs)

    return pl.pallas_call(
        kernel,
        out_shape=(jax.ShapeDtypeStruct(v.shape, BF16), stats),
        in_specs=[VM] * (len(extra) + 4),
        out_specs=(VM, VM),
        scratch_shapes=[pltpu.VMEM((384, 768), BF16), pltpu.VMEM(plane, F32), pltpu.VMEM(plane, F32)],
        compiler_params=params(SPATIAL_MIB),
        cost_estimate=cost(3 * 10**9, 15 * 10**6),
        name="spatial",
    )(*extra, y, v, n, tl)


def final_kernel(pay_ref, energy_ref, u_ref, o_hbm, o_ref, sems):
    def store(g):
        return pltpu.make_async_copy(o_ref.at[chans_of(g)], o_hbm.at[chans_of(g)], sems.at[g])

    target = jnp.sum(pay_ref[...], axis=0)[0:1]
    energy = jnp.sum(energy_ref[...], axis=0)
    scale = jnp.sqrt(target / energy)[0, 0]

    def group(g, _):
        o_ref[chans_of(g)] = (u_ref[chans_of(g)].astype(F32) * scale).astype(BF16)
        store(g).start()
        return 0

    lax.fori_loop(0, GROUPS, group, 0)

    def drain(g, _):
        store(g).wait()
        return 0

    lax.fori_loop(0, GROUPS, drain, 0)


def final_scale(pay, energy, u):
    return pl.pallas_call(
        final_kernel,
        out_shape=jax.ShapeDtypeStruct(u.shape, BF16),
        in_specs=[VM] * 3,
        out_specs=pl.BlockSpec(memory_space=pl.ANY),
        scratch_shapes=[pltpu.VMEM(u.shape, BF16), pltpu.SemaphoreType.DMA((GROUPS,))],
        compiler_params=params(12),
        cost_estimate=cost(10**7, 7 * 10**6),
        name="final_scale",
    )(pay, energy, u)


def swap(x, axes):
    return lax.all_to_all(x, axes, split_axis=0, concat_axis=0, tiled=True)


def ring(x, axis, step):
    n = lax.axis_size(axis)
    return lax.ppermute(x, axis, [(i, (i + step) % n) for i in range(n)])


def stat_parts(stats):
    pair = (stats.astype(F32) + ring(stats, CH[1], 1).astype(F32)).astype(BF16)
    return [pair] + [ring(pair, CH[0], step) for step in range(1, lax.axis_size(CH[0]))]


def per_device(field_in, ln_gain, ln_shift, mix_first, mix_bias, mix_second):
    tf, ti, tw, tl = (jnp.asarray(t) for t in host_tables())
    layers = mix_first.shape[0]
    bias = mix_bias.reshape(layers, 2, -1)
    current, stats = field_in, first_stats(field_in)
    band, scales = None, []
    for layer in range(layers):
        parts = stat_parts(stats)
        if layer == 0:
            normed, lon, band = norm_lon(layer, ln_gain, ln_shift, current, tw, *parts)
        else:
            sums, pay = band_sums(band, parts)
            scales = [swap(pay, LAT)]
            normed, lon = norm_lon(layer, ln_gain, ln_shift, current, tw, *scales, sums)
        back = spectral(layer, swap(lon, LAT), mix_first, bias, mix_second, tf, ti)
        first, last = layer == 0, layer == layers - 1
        current, stats = spatial(first, last, scales, swap(back, LAT), current, normed, tl)
    return final_scale(scales[0], swap(stats, LAT_CH), current)


def solution(mesh):
    finer = Mesh(mesh.devices.reshape(4, 4, 4, 2), LAT_CH)
    in_specs = (
        P(CH, LAT, None),
        P(None, CH),
        P(None, CH),
        P(None, None, CH, None, None),
        P(None, None, CH, None),
        P(None, None, CH, None, None),
    )
    return jax.shard_map(
        per_device, mesh=finer, in_specs=in_specs, out_specs=P(CH, LAT, None), check_vma=False
    )
```
